512 devices in a mesh: tok: 64 (over y, x, core), ch: 8 (over z).
Axes of the slice: x: 4, y: 8, z: 8, core: 2. Of those that a mesh axis runs over, the one named last changes fastest.
Arguments:
- fields: float32 [16384, 1024], P('tok', 'ch'), may hold values from -20 to 20
- gain_one: float32 [1024], P('ch'), may hold values from 0.1 to 1.9
- tok_in_weight: float32 [3072, 16384], P('ch', 'tok'), may hold values from -0.046875 to 0.046875
- tok_in_bias: float32 [3072], P('ch'), may hold values from -3 to 3
- tok_out_weight: float32 [16384, 3072], P('tok', 'ch'), may hold values from -0.109375 to 0.109375
- gain_two: float32 [1024], P('ch'), may hold values from 0.1 to 1.9
- ch_in_weight: float32 [1024, 6144], P('tok', 'ch'), may hold values from -0.1875 to 0.1875
- ch_in_bias: float32 [6144], P('ch'), may hold values from -3 to 3
- ch_out_weight: float32 [6144, 1024], P('ch', 'tok'), may hold values from -0.078125 to 0.078125
Outputs:
- block_out: float32 [16384, 1024], P('tok', 'ch')
The draws below stay inside these ranges and needn't reach their ends.
All inputs are finite; a program needn't handle non-finite values.
Results may differ from the reference program's by a relative error of at most 0.000086.
Values sent between devices are 32-bit elements; how exact they have to be, the bound alone decides.
A program may use at most 64 MiB of HBM per device.

```python
import jax
import jax.numpy as jnp
from jax import lax

TOKENS = 16384
CHANNELS = 1024
TOK_HIDDEN = 3072
CH_HIDDEN = 6144


def draw_fields(key, part):
    key_values, key_scale = jax.random.split(key, 2)
    columns = jnp.arange(CHANNELS, dtype=jnp.float32)
    base_scale = 0.3 * jnp.exp(jnp.log(3.0) * columns / (CHANNELS - 1))
    jitter = jnp.exp(jax.random.uniform(key_scale, (CHANNELS,), jnp.float32, 0.0, jnp.log(3.3)))
    scales = base_scale * jitter
    values = jnp.clip(jax.random.normal(key_values, (TOKENS, CHANNELS), jnp.float32), -6.0, 6.0)
    result = values * scales[None, :]
    return result.astype(jnp.float32)


def shard_levels(own_key, dims, cuts, smallest, largest):
    level = 1.0
    for position, parts in cuts:
        heights = jax.random.uniform(jax.random.fold_in(jax.random.fold_in(own_key, 6), position), (parts,), jnp.float32, smallest / len(cuts), largest / len(cuts))
        level = level * jnp.repeat(jnp.exp(heights), dims[position] // parts).reshape((-1,) + (1,) * (len(dims) - 1 - position))
    return level


def gaussian(rng, dims, scale, most, cuts=(), kind=jnp.bfloat16):
    array = jax.random.normal(rng, dims, jnp.float32) * scale
    if len(cuts) > 0:
        array = shard_levels(rng, dims, cuts, -0.22, 0.18) * array
    return jnp.clip(array, min=-most, max=most).astype(kind)


def setup_inputs(seed: int = 0) -> dict:
    streams_of = jax.random.split(jax.random.key(seed), 10)
    return {
        "fields": draw_fields(jax.random.fold_in(streams_of[9], 71), 0),
        "gain_one": jnp.clip(1.0 + 0.18 * jax.random.normal(streams_of[1], (CHANNELS,), jnp.float32), 0.1, 1.9),
        "tok_in_weight": gaussian(streams_of[2], (TOK_HIDDEN, TOKENS), TOKENS ** -0.5, 0.046875, ((0, 8), (1, 64)), jnp.float32),
        "tok_in_bias": gaussian(streams_of[3], (TOK_HIDDEN,), 0.5, 3.0, ((0, 8),), jnp.float32),
        "tok_out_weight": gaussian(streams_of[4], (TOKENS, TOK_HIDDEN), TOK_HIDDEN ** -0.5, 0.109375, ((0, 64), (1, 8)), jnp.float32),
        "gain_two": jnp.clip(1.0 + 0.18 * jax.random.normal(streams_of[5], (CHANNELS,), jnp.float32), 0.1, 1.9),
        "ch_in_weight": gaussian(streams_of[6], (CHANNELS, CH_HIDDEN), CHANNELS ** -0.5, 0.1875, ((0, 64), (1, 8)), jnp.float32),
        "ch_in_bias": gaussian(streams_of[7], (CH_HIDDEN,), 0.5, 3.0, ((0, 8),), jnp.float32),
        "ch_out_weight": gaussian(streams_of[8], (CH_HIDDEN, CHANNELS), CH_HIDDEN ** -0.5, 0.078125, ((0, 8), (1, 64)), jnp.float32),
    }


epsilon = 1e-05

def layer_norm(values, gain):
    centre = lax.optimization_barrier(jnp.mean(values, axis=-1, keepdims=True))
    centred = values - centre
    spread = lax.optimization_barrier(jnp.mean(centred * centred, axis=-1, keepdims=True))
    return centred * lax.rsqrt(spread + epsilon) * gain

def matmul(left, right):
    return jnp.dot(left, right, precision=lax.Precision.HIGHEST, preferred_element_type=jnp.float32)

def reference(fields, gain_one, tok_in_weight, tok_in_bias, tok_out_weight, gain_two, ch_in_weight, ch_in_bias, ch_out_weight):
    normed = layer_norm(fields, gain_one)
    hidden_tok = jax.nn.gelu(matmul(tok_in_weight, normed) + tok_in_bias[:, None], approximate=False)
    mixed_tok = fields + matmul(tok_out_weight, hidden_tok)
    normed_two = layer_norm(mixed_tok, gain_two)
    hidden_ch = jax.nn.gelu(matmul(normed_two, ch_in_weight) + ch_in_bias[None, :], approximate=False)
    return mixed_tok + matmul(hidden_ch, ch_out_weight)
```

```python
import functools

import jax
import jax.numpy as jnp
from jax import lax
from jax.experimental import pallas as pl
from jax.experimental.pallas import tpu as pltpu
from jax.sharding import PartitionSpec as P

NY, NX = 8, 4
CORES = 2
MESH = pl.DeviceIdType.MESH
F32, BF16 = jnp.float32, jnp.bfloat16
EPSILON = 1e-05
LANES = 128


def split(value):
    high = value.astype(BF16)
    return high, (value - high.astype(F32)).astype(BF16)


def gelu(value):
    return 0.5 * value * (1.0 + lax.erf(value * 0.7071067811865476))


def dot3(a_high, a_low, b_high, b_low, dims):
    def one(a, b):
        return lax.dot_general(a, b, (dims, ((), ())), preferred_element_type=F32)

    return one(a_high, b_high) + (one(a_high, b_low) + one(a_low, b_high))


NN = ((1,), (0,))
NT = ((1,), (1,))


class Sender:
    def __init__(self, send_sem, recv_sem):
        self.send_sem, self.recv_sem = send_sem, recv_sem
        self.copies = []

    def __call__(self, src, dst, device):
        k = len(self.copies)
        copy = pltpu.make_async_remote_copy(
            src_ref=src,
            dst_ref=dst,
            send_sem=self.send_sem.at[k],
            recv_sem=self.recv_sem.at[k],
            device_id=device,
            device_id_type=MESH,
        )
        copy.start()
        self.copies.append(copy)
        return copy

    def finish(self):
        for copy in self.copies:
            copy.wait_send()


def wrap(value, n):
    return lax.rem(value + 2 * n, n)


def gather_ring(n, me, device, view, send, arrived=lambda src, h: None):
    half = n // 2
    flight = {}

    def take(d, s, h):
        flight.pop((d, s, h)).wait_recv()
        arrived(wrap(me - d * s, n), h)

    for s in range(1, half + 1):
        for h in (0, 1):
            for d in (1, -1):
                if s == half and (d == 1) != (h == 0):
                    continue
                if s > 1:
                    take(d, s - 1, h)
                block = view(wrap(me - d * (s - 1), n), h)
                flight[(d, s, h)] = send(block, block, device(wrap(me + d, n)))
        yield
    for key in sorted(flight, key=lambda k: (k[1], k[2])):
        take(*key)
    yield


def reduce_ring(n, me, device, part, slot, send, ready=lambda dst, dist: None):
    half = n // 2
    flight = {}

    def add(dst, d, t, h):
        flight.pop((d, t, h)).wait_recv()
        part(dst, h)[...] += slot(d, t, h)[...]

    for t in range(1, half + 1):
        dist = half + 1 - t
        ready(wrap(me + dist, n), dist)
        if dist != half:
            ready(wrap(me - dist, n), -dist)
        for h in (0, 1):
            for d in (1, -1):
                first = 1 if (d == 1) == (h == 0) else 2
                if t < first:
                    continue
                dst = wrap(me + d * dist, n)
                if t > first:
                    add(dst, d, t - 1, h)
                flight[(d, t, h)] = send(part(dst, h), slot(d, t, h), device(wrap(me + d, n)))
        yield
    ready(me, 0)
    for key in sorted(flight, key=lambda k: (k[1], k[2])):
        add(me, *key)
    yield


def slots_of(n):
    half = n // 2
    places = {}
    for t in range(1, half + 1):
        for h in (0, 1):
            for d in (1, -1):
                if t >= (1 if (d == 1) == (h == 0) else 2):
                    places[(d, t, h)] = len(places)
    return places


def kernel(
    nz, ny, nx,
    fields, gain_one, gain_two, tok_in, tok_bias, tok_out, ch_in, ch_bias, ch_out,
    out,
    gathered, kept, high, low, tok_in_f, tok_in_h, tok_in_l, tok_out_f, tok_out_h, tok_out_l,
    sums, sums_pair, sums_slot, sums_x, hidden, hidden_h, hidden_l,
    mixed, mixed_slot, ch_in_f, ch_in_h, ch_in_l, ch_out_f, ch_out_h, ch_out_l, act_h, act_l,
    final, final_slot, local_sem, send_sem, recv_sem,
):
    tok, z = lax.axis_index("tok"), lax.axis_index("ch")
    core = lax.rem(tok, CORES)
    chip = lax.div(tok, CORES)
    x, y = lax.rem(chip, nx), lax.div(chip, nx)
    rows = fields.shape[0]
    half_rows = rows // 2
    channels = nz * LANES
    x_width = channels // nx
    per_x = x_width // LANES
    y_rows = sums.shape[3]
    core_rows = ny * y_rows
    hidden_width = ch_in.shape[1]
    depth = ch_in.shape[0]

    def at_z(i):
        return (tok, i)

    def at_y(i):
        return ((i * nx + x) * CORES + core, z)

    def at_x(i):
        return ((y * nx + i) * CORES + core, z)

    partner = ((y * nx + x) * CORES + (1 - core), z)

    local = [
        pltpu.make_async_copy(fields, gathered.at[z, pl.ds(0, rows)], local_sem.at[0]),
        pltpu.make_async_copy(gain_one, gathered.at[z, pl.ds(rows, 1)], local_sem.at[1]),
        pltpu.make_async_copy(gain_two, gathered.at[z, pl.ds(rows + 1, 1)], local_sem.at[2]),
        pltpu.make_async_copy(ch_in, ch_in_f.at[core, y, x], local_sem.at[3]),
        pltpu.make_async_copy(ch_out, ch_out_f.at[core, x, y], local_sem.at[4]),
        pltpu.make_async_copy(tok_in, tok_in_f, local_sem.at[5]),
        pltpu.make_async_copy(tok_out, tok_out_f, local_sem.at[6]),
    ]
    for copy in local:
        copy.start()

    peers = [partner]
    if nz > 1:
        peers += [at_z(wrap(z + 1, nz)), at_z(wrap(z - 1, nz))]
    if ny > 1:
        peers += [at_y(wrap(y + 1, ny)), at_y(wrap(y - 1, ny))]
    peers += [at_x(wrap(x + k, nx)) for k in range(1, nx)]
    barrier = pltpu.get_barrier_semaphore()
    for peer in peers:
        pl.semaphore_signal(barrier, inc=1, device_id=peer, device_id_type=MESH)
    for copy in local[:5]:
        copy.wait()
    pl.semaphore_wait(barrier, len(peers))

    send = Sender(send_sem, recv_sem)

    def field_view(src, h):
        if h == 0:
            return gathered.at[src, pl.ds(0, half_rows)]
        return gathered.at[src, pl.ds(half_rows, half_rows + 8)]

    half_depth = depth // 2
    ring_fields = gather_ring(nz, z, at_z, field_view, send)
    ring_out_y = gather_ring(
        ny, y, at_y, lambda src, h: ch_out_f.at[core, x, src, pl.ds(h * half_depth, half_depth)], send
    )

    def in_to_partner(src, h):
        block = ch_in_f.at[core, src, :, pl.ds(h * half_depth, half_depth)]
        pair_copies.append(send(block, block, partner))

    def out_to_partner(src, h):
        block = ch_out_f.at[core, src, :, pl.ds(h * half_depth, half_depth)]
        pair_copies.append(send(block, block, partner))

    pair_copies = []
    ring_in_y = gather_ring(
        ny, y, at_y, lambda src, h: ch_in_f.at[core, src, :, pl.ds(h * half_depth, half_depth)], send, in_to_partner
    )
    ring_out_x = gather_ring(
        nx, x, at_x, lambda src, h: ch_out_f.at[core, src, :, pl.ds(h * half_depth, half_depth)], send, out_to_partner
    )

    next(ring_fields)
    own = ch_in_f.at[core, y, x]
    in_x = [send(own, own, at_x(wrap(x + k, nx))) for k in range(1, nx)]
    next(ring_out_y, None)
    for copy in local[5:]:
        copy.wait()

    def split_rows(source, high_ref, low_ref, step=32):
        def body(i, _):
            at = pl.ds(pl.multiple_of(i * step, step), step)
            high_ref[at, :], low_ref[at, :] = split(source[at, :])
            return 0

        lax.fori_loop(0, source.shape[0] // step, body, 0)

    split_rows(tok_in_f, tok_in_h, tok_in_l)
    split_rows(tok_out_f, tok_out_h, tok_out_l)
    for _ in ring_fields:
        next(ring_out_y, None)
    for _ in ring_out_y:
        pass
    for copy in in_x:
        copy.wait_recv()
    for h in (0, 1):
        in_to_partner(y, h)
        out_to_partner(x, h)
    next(ring_in_y)
    next(ring_out_x)

    def normalize(source, gain_row):
        step = 32

        def body(i, _):
            at = pl.ds(pl.multiple_of(i * step, step), step)
            blocks = [source[j, at, :] for j in range(nz)]
            mean = jnp.sum(sum(blocks[1:], blocks[0]), axis=1, keepdims=True) * (1.0 / channels)
            centred = [block - mean for block in blocks]
            squares = [block * block for block in centred]
            spread = jnp.sum(sum(squares[1:], squares[0]), axis=1, keepdims=True) * (1.0 / channels)
            scale = lax.rsqrt(spread + EPSILON)
            for j in range(nz):
                gain = gathered[j, pl.ds(gain_row, 1), :]
                columns = pl.ds(j * LANES, LANES)
                high[at, columns], low[at, columns] = split(centred[j] * scale * gain)
            return 0

        lax.fori_loop(0, rows // step, body, 0)

    normalize(gathered, rows)

    def hidden_sums(which):
        at = pl.ds(pl.multiple_of(which * core_rows, core_rows), core_rows)

        def body(j, _):
            columns = pl.ds(pl.multiple_of(j * x_width, x_width), x_width)
            result = dot3(tok_in_h[at, :], tok_in_l[at, :], high[:, columns], low[:, columns], NN)
            for i in range(ny):
                sums[which, i, j] = result[i * y_rows : (i + 1) * y_rows]
            return 0

        lax.fori_loop(0, nx, body, 0)

    half_y = ny // 2
    offsets = [half_y] if half_y else []
    for dist in range(half_y - 1, 0, -1):
        offsets += [dist, -dist]
    offsets.append(0)
    hidden_sums(1 - core)
    pair_sums = {}
    for k in offsets:
        dst = wrap(y + k, ny)
        pair_sums[k] = send(sums.at[1 - core, dst], sums_pair.at[dst], partner)
    hidden_sums(core)

    def sums_ready(dst, dist):
        pair_sums[dist].wait_recv()
        sums[core, dst] += sums_pair[dst]

    half_x = nx // 2
    y_slots = slots_of(ny)
    for _ in reduce_ring(
        ny,
        y,
        at_y,
        lambda dst, h: sums.at[core, dst, pl.ds(h * half_x, half_x)],
        lambda d, t, h: sums_slot.at[y_slots[(d, t, h)]],
        send,
        sums_ready,
    ):
        pass
    copies = []
    for k in range(1, nx):
        dst = wrap(x + k, nx)
        copies.append(send(sums.at[core, y, dst], sums_x.at[k - 1], at_x(dst)))
    total = sums[core, y, x]
    for k, copy in enumerate(copies):
        copy.wait_recv()
        total = total + sums_x[k]
    first = core * core_rows + y * y_rows
    shape = (y_rows, tok_bias.shape[1])
    wanted = lax.broadcasted_iota(jnp.int32, shape, 1) == lax.broadcasted_iota(jnp.int32, shape, 0) + first
    bias = jnp.sum(jnp.where(wanted, jnp.broadcast_to(tok_bias[...], shape), 0.0), axis=1, keepdims=True)
    hidden[core, y, x] = gelu(total + bias)

    own = hidden.at[core, y, x]
    copies = [send(own, own, at_x(wrap(x + k, nx))) for k in range(1, nx)]
    for copy in copies:
        copy.wait_recv()
    pair_hidden = []

    def hidden_view(src, h):
        return hidden.at[core, src, pl.ds(h * half_x, half_x)]

    def hidden_to_partner(src, h):
        block = hidden_view(src, h)
        pair_hidden.append(send(block, block, partner))

    ring = gather_ring(ny, y, at_y, hidden_view, send, hidden_to_partner)
    next(ring)
    for h in (0, 1):
        hidden_to_partner(y, h)
    for _ in ring:
        pass
    for copy in pair_hidden:
        copy.wait_recv()
    for c in range(CORES):

        def split_hidden(j, _):
            value = hidden[c, :, j].reshape(core_rows, x_width)
            for k in range(per_x):
                pair = split(value[:, k * LANES : (k + 1) * LANES])
                hidden_h[j * per_x + k, pl.ds(c * core_rows, core_rows)] = pair[0]
                hidden_l[j * per_x + k, pl.ds(c * core_rows, core_rows)] = pair[1]
            return 0

        lax.fori_loop(0, nx, split_hidden, 0)

    def mixed_ready(dst, dist):
        mixed[dst] = dot3(tok_out_h[...], tok_out_l[...], hidden_h[dst], hidden_l[dst], NN)

    z_slots = slots_of(nz)

    def row_half(ref):
        return lambda i, h: ref.at[i, pl.ds(h * half_rows, half_rows)]

    ring = reduce_ring(
        nz, z, at_z, row_half(mixed), lambda d, t, h: mixed_slot.at[z_slots[(d, t, h)]], send, mixed_ready
    )
    for k, _ in enumerate(ring):
        if k % 2 == 0:
            next(ring_in_y, None)
        else:
            next(ring_out_x, None)
    kept[z] = gathered[z, pl.ds(0, rows), :] + mixed[z]
    ring = gather_ring(nz, z, at_z, row_half(kept), send)
    for k, _ in enumerate(ring):
        if k % 2 == 0:
            next(ring_in_y, None)
        else:
            next(ring_out_x, None)
    for late in (ring_in_y, ring_out_x):
        for _ in late:
            pass
    for copy in pair_copies:
        copy.wait_recv()

    def split_weights(i, _):
        for c in range(CORES):
            for j in range(nx):
                row = ((i * nx + j) * CORES + c) * depth
                at = pl.ds(pl.multiple_of(row, depth), depth)
                ch_in_h[at, :], ch_in_l[at, :] = split(ch_in_f[c, i, j])
                ch_out_h[at, :], ch_out_l[at, :] = split(ch_out_f[c, j, i])
        return 0

    lax.fori_loop(0, ny, split_weights, 0)
    normalize(kept, rows + 1)

    width = 256

    def hidden_block(j, _):
        columns = pl.ds(pl.multiple_of(j * width, width), width)
        result = dot3(high[...], low[...], ch_in_h[:, columns], ch_in_l[:, columns], NN)
        act_h[:, columns], act_l[:, columns] = split(gelu(result + ch_bias[:, columns]))
        return 0

    lax.fori_loop(0, hidden_width // width, hidden_block, 0)

    def final_ready(dst, dist):
        at = pl.ds(pl.multiple_of(dst * LANES, LANES), LANES)
        final[dst] = dot3(act_h[...], act_l[...], ch_out_h[at, :], ch_out_l[at, :], NT)

    for _ in reduce_ring(
        nz, z, at_z, row_half(final), lambda d, t, h: final_slot.at[z_slots[(d, t, h)]], send, final_ready
    ):
        pass
    out[...] = kept[z] + final[z]
    send.finish()


COPIES = 256


def block(nz, ny, nx, fields, gain_one, tok_in, tok_bias, tok_out, gain_two, ch_in, ch_bias, ch_out):
    rows, hidden_tok = fields.shape[0], tok_in.shape[0]
    depth, hidden_width = ch_in.shape
    channels = nz * LANES
    y_rows = hidden_tok // (CORES * ny)
    x_width = channels // nx
    z_slots, y_slots = max(1, len(slots_of(nz))), max(1, len(slots_of(ny)))

    def vmem(*shape, kind=F32):
        return pltpu.VMEM(shape, kind)

    scratch = [
        vmem(nz, rows + 8, LANES),
        vmem(nz, rows, LANES),
        vmem(rows, channels, kind=BF16),
        vmem(rows, channels, kind=BF16),
        vmem(hidden_tok, rows),
        vmem(hidden_tok, rows, kind=BF16),
        vmem(hidden_tok, rows, kind=BF16),
        vmem(rows, hidden_tok),
        vmem(rows, hidden_tok, kind=BF16),
        vmem(rows, hidden_tok, kind=BF16),
        vmem(CORES, ny, nx, y_rows, x_width),
        vmem(ny, nx, y_rows, x_width),
        vmem(y_slots, nx // 2, y_rows, x_width),
        vmem(nx - 1, y_rows, x_width),
        vmem(CORES, ny, nx, y_rows, x_width),
        vmem(nz, hidden_tok, LANES, kind=BF16),
        vmem(nz, hidden_tok, LANES, kind=BF16),
        vmem(nz, rows, LANES),
        vmem(z_slots, rows // 2, LANES),
        vmem(CORES, ny, nx, depth, hidden_width),
        vmem(channels, hidden_width, kind=BF16),
        vmem(channels, hidden_width, kind=BF16),
        vmem(CORES, nx, ny, depth, hidden_width),
        vmem(channels, hidden_width, kind=BF16),
        vmem(channels, hidden_width, kind=BF16),
        vmem(rows, hidden_width, kind=BF16),
        vmem(rows, hidden_width, kind=BF16),
        vmem(nz, rows, LANES),
        vmem(z_slots, rows // 2, LANES),
        pltpu.SemaphoreType.DMA((7,)),
        pltpu.SemaphoreType.DMA((COPIES,)),
        pltpu.SemaphoreType.DMA((COPIES,)),
    ]
    hbm, near = pl.BlockSpec(memory_space=pl.ANY), pl.BlockSpec(memory_space=pltpu.VMEM)
    return pl.pallas_call(
        functools.partial(kernel, nz, ny, nx),
        out_shape=jax.ShapeDtypeStruct((rows, LANES), F32),
        in_specs=[hbm, hbm, hbm, hbm, near, hbm, hbm, near, hbm],
        out_specs=near,
        scratch_shapes=scratch,
        compiler_params=pltpu.CompilerParams(
            collective_id=0, has_side_effects=True, vmem_limit_bytes=48 * 1024 * 1024
        ),
    )(
        fields,
        gain_one.reshape(1, LANES),
        gain_two.reshape(1, LANES),
        tok_in,
        tok_bias.reshape(1, hidden_tok),
        tok_out,
        ch_in,
        ch_bias.reshape(1, hidden_width),
        ch_out.T,
    )


def solution(mesh):
    in_specs = (
        P("tok", "ch"),
        P("ch"),
        P("ch", "tok"),
        P("ch"),
        P("tok", "ch"),
        P("ch"),
        P("tok", "ch"),
        P("ch"),
        P("ch", "tok"),
    )
    body = functools.partial(block, mesh.shape["ch"], NY, NX)
    return jax.shard_map(body, mesh=mesh, in_specs=in_specs, out_specs=P("tok", "ch"), check_vma=False)
```

```python
import functools

import jax
import jax.numpy as jnp
from jax import lax
from jax.experimental import pallas as pl
from jax.experimental.pallas import tpu as pltpu
from jax.sharding import PartitionSpec as P

NY, NX = 8, 4
CORES = 2
CHUNKS = 2
PIECES = 4
MESH = pl.DeviceIdType.MESH
F32, BF16 = jnp.float32, jnp.bfloat16
EPSILON = 1e-05
LANES = 128
GAINS = 8


def split(value):
    high = value.astype(BF16)
    return high, (value - high.astype(F32)).astype(BF16)


def gelu(value):
    return 0.5 * value * (1.0 + lax.erf(value * 0.7071067811865476))


def dot3(a_high, a_low, b_high, b_low, dims):
    def one(a, b):
        return lax.dot_general(a, b, (dims, ((), ())), preferred_element_type=F32)

    return one(a_high, b_high) + (one(a_high, b_low) + one(a_low, b_high))


NN = ((1,), (0,))
NT = ((1,), (1,))
SENDS, RECEIVES = 22, 299


class Sender:
    def __init__(self, send_sem, recv_sem):
        self.send_sem, self.recv_sem = send_sem, recv_sem
        self.groups, self.receives = {}, 0

    def receive(self):
        self.receives += 1
        return self.recv_sem.at[self.receives - 1]

    def __call__(self, group, src, dst, device, recv=None):
        copy = pltpu.make_async_remote_copy(
            src_ref=src,
            dst_ref=dst,
            send_sem=self.send_sem.at[self.groups.setdefault(group, len(self.groups))],
            recv_sem=self.receive() if recv is None else recv,
            device_id=device,
            device_id_type=MESH,
        )
        copy.start()
        return copy

    def finish(self, sizes):
        for group, k in self.groups.items():
            wait_for(sizes[group], self.send_sem.at[k])


def wait_for(like, sem):
    pltpu.make_async_copy(like, like, sem).wait()


def wrap(value, n):
    return lax.rem(value + 2 * n, n)


def gather_ring(n, me, device, view, send, group, arrived=lambda src, h: None, pieces=2):
    half = n // 2
    flight = {}

    def take(d, s, h):
        flight.pop((d, s, h)).wait_recv()
        arrived(wrap(me - d * s, n), h)

    for s in range(1, half + 1):
        for h in range(pieces):
            for d in (1, -1):
                if s == half and (d == 1) != (h < pieces // 2):
                    continue
                if s > 1:
                    take(d, s - 1, h)
                block = view(wrap(me - d * (s - 1), n), h)
                flight[(d, s, h)] = send(group, block, block, device(wrap(me + d, n)))
        yield
    for key in sorted(flight, key=lambda k: (k[1], k[2])):
        take(*key)


def reduce_ring(n, me, device, part, slot, send, group, ready=lambda dst, dist: None, pieces=2):
    half = n // 2
    flight = {}

    def add(dst, d, t, h):
        flight.pop((d, t, h)).wait_recv()
        part(dst, h)[...] += slot(d, t, h)[...]

    for t in range(1, half + 1):
        dist = half + 1 - t
        ready(wrap(me + dist, n), dist)
        if dist != half:
            ready(wrap(me - dist, n), -dist)
        for h in range(pieces):
            for d in (1, -1):
                first = 1 if (d == 1) == (h < pieces // 2) else 2
                if t < first:
                    continue
                dst = wrap(me + d * dist, n)
                if t > first:
                    add(dst, d, t - 1, h)
                flight[(d, t, h)] = send(group, part(dst, h), slot(d, t, h), device(wrap(me + d, n)))
        yield
    ready(me, 0)
    for key in sorted(flight, key=lambda k: (k[1], k[2])):
        add(me, *key)


def reduce_two_stages(me, device, whole, half, slot, send, group, ready):
    n = 8
    flight = {}
    ready(wrap(me + 4, n), 4)
    for d in (1, -1):
        dst = wrap(me + 4 * d, n)
        flight[(d, 4)] = send(group, half(dst, d), slot(d, 4), device(wrap(me + 2 * d, n)))
    for d in (1, -1):
        dst = wrap(me + 3 * d, n)
        ready(dst, 3 * d)
        flight[(d, 3)] = send(group, whole(dst), slot(d, 3), device(wrap(me + d, n)))
    for d in (1, -1):
        dst = wrap(me + d, n)
        ready(dst, d)
        flight[(d, 1)] = send(group, whole(dst), slot(d, 1), device(dst))
    for d in (1, -1):
        ready(wrap(me + 2 * d, n), 2 * d)
    ready(me, 0)
    yield
    for d in (1, -1):
        dst = wrap(me + 2 * d, n)
        flight[(d, 3)].wait_recv()
        flight[(d, 4)].wait_recv()
        whole(dst)[...] += slot(d, 3)[...]
        half(dst, d)[...] += slot(d, 4)[...]
        flight[(d, 2)] = send(group, whole(dst), slot(d, 2), device(dst))
    yield
    for k in (1, 2):
        for d in (1, -1):
            flight[(d, k)].wait_recv()
            whole(me)[...] += slot(d, k)[...]


def gather_two_stages(me, device, whole, half, send, group, arrived):
    n = 8
    flight = {}
    own = whole(me)
    for k in (2, 1):
        for d in (1, -1):
            flight[(d, k)] = send(group, own, own, device(wrap(me + k * d, n)))
    yield
    for d in (1, -1):
        src = wrap(me - 2 * d, n)
        flight[(d, 2)].wait_recv()
        block = half(src, d)
        flight[(d, 4)] = send(group, block, block, device(wrap(me + 2 * d, n)))
        block = whole(src)
        flight[(d, 3)] = send(group, block, block, device(wrap(me + d, n)))
        arrived(block)
    for d in (1, -1):
        flight[(d, 1)].wait_recv()
        arrived(whole(wrap(me - d, n)))
    yield
    for d in (1, -1):
        flight[(d, 3)].wait_recv()
        arrived(whole(wrap(me - 3 * d, n)))
    for d in (1, -1):
        flight[(d, 4)].wait_recv()
        arrived(half(wrap(me - 4 * d, n), d))


def slots_of(n, pieces=2):
    half = n // 2
    places = {}
    for t in range(1, half + 1):
        for h in range(pieces):
            for d in (1, -1):
                if t >= (1 if (d == 1) == (h < pieces // 2) else 2):
                    places[(d, t, h)] = len(places)
    return places


def kernel(
    nz, ny, nx,
    fields, gain_one, gain_two, tok_in, tok_bias, tok_out, ch_in, ch_bias, ch_out,
    out,
    gathered, kept, high, low, tok_in_f, tok_in_h, tok_in_l, tok_out_f, tok_out_h, tok_out_l,
    sums_a, sums_b, pair_a, pair_b, slot_a, slot_ax, slot_bx, slot_by, hidden_a, hidden_b, hidden_h, hidden_l,
    mixed, mixed_slot, ch_in_f, ch_in_h, ch_in_l, ch_out_f, ch_out_h, ch_out_l, act_h, act_l,
    final, final_slot, tok_bias_v, ch_bias_v, local_sem, send_sem, recv_sem,
):
    tok, z = lax.axis_index("tok"), lax.axis_index("ch")
    core = lax.rem(tok, CORES)
    chip = lax.div(tok, CORES)
    x, y = lax.rem(chip, nx), lax.div(chip, nx)
    other = 1 - core
    rows = fields.shape[0]
    chunk_rows = rows // CHUNKS
    piece_rows = chunk_rows // PIECES
    channels = nz * LANES
    x_width = sums_a.shape[4]
    per_x = x_width // LANES
    y_rows = sums_a.shape[3]
    core_rows = ny * y_rows
    depth, hidden_width = ch_in.shape
    half_x, half_y = nx // 2, ny // 2

    def at_z(i):
        return (tok, i)

    def at_y(i):
        return ((i * nx + x) * CORES + core, z)

    def at_x(i):
        return ((y * nx + i) * CORES + core, z)

    partner = ((y * nx + x) * CORES + other, z)
    others_x = [wrap(x + k, nx) for k in range(1, nx)]
    others_y = [wrap(y + k, ny) for k in range(1, ny)]

    local = [
        pltpu.make_async_copy(source, target, local_sem.at[k])
        for k, (source, target) in enumerate(
            [
                (fields, gathered.at[z, pl.ds(GAINS, rows)]),
                (gain_one, gathered.at[z, pl.ds(0, 1)]),
                (gain_two, gathered.at[z, pl.ds(1, 1)]),
                (ch_in, ch_in_f.at[core, y, x]),
                (ch_out, ch_out_f.at[core, x, y]),
                (tok_in, tok_in_f),
                (tok_out, tok_out_f),
                (tok_bias, tok_bias_v.at[0]),
                (ch_bias, ch_bias_v.at[0]),
            ]
        )
    ]
    for copy in local:
        copy.start()

    peers = [partner] + [at_x(i) for i in others_x] + [at_y(i) for i in others_y]
    if nz > 1:
        peers += [at_z(wrap(z + 1, nz)), at_z(wrap(z - 1, nz))]
    barrier = pltpu.get_barrier_semaphore()
    for peer in peers:
        pl.semaphore_signal(barrier, inc=1, device_id=peer, device_id_type=MESH)
    for copy in local[:5]:
        copy.wait()
    pl.semaphore_wait(barrier, len(peers))

    send = Sender(send_sem, recv_sem)

    def field_view(c):
        def view(src, h):
            start = c * chunk_rows + h * piece_rows
            if start == 0:
                return gathered.at[src, pl.ds(0, piece_rows + GAINS)]
            return gathered.at[src, pl.ds(start + GAINS, piece_rows)]

        return view

    half_depth = depth // 2

    def depth_half(ref):
        return lambda src, h: ref.at[core, src, :, pl.ds(h * half_depth, half_depth)]

    pair_in_sem, pair_out_sem = send.receive(), send.receive()

    def in_to_partner(src, h):
        block = depth_half(ch_in_f)(src, h)
        send("pair in", block, block, partner, pair_in_sem)

    def out_to_partner(src, h):
        block = depth_half(ch_out_f)(src, h)
        send("pair out", block, block, partner, pair_out_sem)

    ring_fields = [gather_ring(nz, z, at_z, field_view(c), send, "fields", pieces=PIECES) for c in range(CHUNKS)]
    ring_out_y = gather_ring(
        ny, y, at_y, lambda src, h: ch_out_f.at[core, x, src, pl.ds(h * half_depth, half_depth)], send, "out y"
    )
    ring_in_y = gather_ring(ny, y, at_y, depth_half(ch_in_f), send, "in y", in_to_partner)
    ring_out_x = gather_ring(nx, x, at_x, depth_half(ch_out_f), send, "out x", out_to_partner)

    for ring in ring_fields:
        next(ring, None)
    own = ch_in_f.at[core, y, x]
    in_x_sem = send.receive()
    for i in others_x:
        send("in x", own, own, at_x(i), in_x_sem)
    next(ring_out_y, None)
    for copy in local[5:]:
        copy.wait()

    def split_rows(source, high_ref, low_ref, step=32):
        def body(i, _):
            at = pl.ds(pl.multiple_of(i * step, step), step)
            high_ref[at, :], low_ref[at, :] = split(source[at, :])
            return 0

        lax.fori_loop(0, source.shape[0] // step, body, 0)

    split_rows(tok_in_f, tok_in_h, tok_in_l)
    split_rows(tok_out_f, tok_out_h, tok_out_l)

    def normalize(c, source, offset, gain_row):
        step = 32

        def body(i, _):
            row = c * chunk_rows + i * step
            at = pl.ds(pl.multiple_of(row, step), step)
            blocks = [source[j, pl.ds(pl.multiple_of(row + offset, 8), step), :] for j in range(nz)]
            mean = jnp.sum(sum(blocks[1:], blocks[0]), axis=1, keepdims=True) * (1.0 / channels)
            centred = [block - mean for block in blocks]
            squares = [block * block for block in centred]
            spread = jnp.sum(sum(squares[1:], squares[0]), axis=1, keepdims=True) * (1.0 / channels)
            scale = lax.rsqrt(spread + EPSILON)
            for j in range(nz):
                gain = gathered[j, pl.ds(gain_row, 1), :]
                columns = pl.ds(j * LANES, LANES)
                high[at, columns], low[at, columns] = split(centred[j] * scale * gain)
            return 0

        lax.fori_loop(0, chunk_rows // step, body, 0)

    for s in range(2, nz // 2 + 1):
        for ring in ring_fields:
            next(ring)
        next(ring_out_y, None)
    for c, ring in enumerate(ring_fields):
        for _ in ring:
            pass
        if c == CHUNKS - 1:
            for _ in ring_out_y:
                pass
            if nx > 1:
                wait_for(ch_in_f.at[0, 0, pl.ds(0, nx - 1)], in_x_sem)
            for h in (0, 1):
                in_to_partner(y, h)
                out_to_partner(x, h)
            next(ring_in_y, None)
            next(ring_out_x, None)
        normalize(c, gathered, GAINS, 0)

    def hidden_sums(which, i):
        at = pl.ds(pl.multiple_of(which * core_rows, core_rows), core_rows)

        def body(j, _):
            start = i * (channels // 2) + 2 * j * x_width
            columns = pl.ds(pl.multiple_of(start, LANES), 2 * x_width)
            result = dot3(tok_in_h[at, :], tok_in_l[at, :], high[:, columns], low[:, columns], NN)
            for k in range(2):
                for r in range(ny):
                    piece = result[r * y_rows : (r + 1) * y_rows, k * x_width : (k + 1) * x_width]
                    if i == 0:
                        sums_a[which, r, 2 * j + k] = piece
                    else:
                        sums_b[which, 2 * j + k, r] = piece
            return 0

        lax.fori_loop(0, half_x, body, 0)

    offsets = [4, 3, -3, 1, -1, 2, -2, 0] if ny == 8 else [0]
    if ny != 8:
        for dist in range(1, half_y):
            offsets = [dist, -dist] + offsets
        offsets = ([half_y] if half_y else []) + offsets
    hidden_sums(other, 0)
    pair_sums = {}
    for k in offsets:
        dst = wrap(y + k, ny)
        pair_sums[k] = send("pair a", sums_a.at[other, dst], pair_a.at[dst], partner)
    hidden_sums(other, 1)
    pair_b_copies = []
    for i in others_x + [x]:
        pair_b_copies.append(send("pair b", sums_b.at[other, i], pair_b.at[i], partner))
    hidden_sums(core, 0)
    hidden_sums(core, 1)

    def sums_ready(dst, dist):
        pair_sums[dist].wait_recv()
        sums_a[core, dst] += pair_a[dst]

    y_slots = slots_of(ny)

    def sums_half(dst, h):
        return sums_a.at[core, dst, pl.ds(h * half_x, half_x)]

    if ny == 8:
        places = {1: 0, 2: 2, 3: 4}

        def y_slot(d, k):
            if k == 4:
                return slot_a.at[6, pl.ds((d < 0) * half_x, half_x)]
            return slot_a.at[places[k] + (d < 0)]

        ring = reduce_two_stages(
            y,
            at_y,
            lambda dst: sums_a.at[core, dst],
            lambda dst, d: sums_half(dst, int(d < 0)),
            y_slot,
            send,
            "sums y",
            sums_ready,
        )
    else:
        ring = reduce_ring(
            ny,
            y,
            at_y,
            sums_half,
            lambda d, t, h: slot_a.at[y_slots[(d, t, h)] // 2, pl.ds((y_slots[(d, t, h)] % 2) * half_x, half_x)],
            send,
            "sums y",
            sums_ready,
        )
    next(ring, None)
    bx_sem, by_sem, ax_sem = send.receive(), send.receive(), send.receive()
    for k, i in enumerate(others_x):
        pair_b_copies[k].wait_recv()
        sums_b[core, i] += pair_b[i]
        send("b x", sums_b.at[core, i], slot_bx.at[k], at_x(i), bx_sem)
    pair_b_copies[-1].wait_recv()
    sums_b[core, x] += pair_b[x]
    next(ring, None)
    if nx > 1:
        wait_for(slot_bx, bx_sem)

    def add_bx(r, _):
        total = sums_b[core, x, r]
        for k in range(nx - 1):
            total = total + slot_bx[k, r]
        sums_b[core, x, r] = total
        return 0

    lax.fori_loop(0, ny, add_bx, 0)
    for k, i in enumerate(others_y):
        send("b y", sums_b.at[core, x, i], slot_by.at[k], at_y(i), by_sem)
    for _ in ring:
        pass
    for k, i in enumerate(others_x):
        send("a x", sums_a.at[core, y, i], slot_ax.at[k], at_x(i), ax_sem)
    first = core * core_rows + y * y_rows
    shape = (y_rows, tok_bias_v.shape[1])
    wanted = lax.broadcasted_iota(jnp.int32, shape, 1) == lax.broadcasted_iota(jnp.int32, shape, 0) + first
    bias = jnp.sum(jnp.where(wanted, jnp.broadcast_to(tok_bias_v[...], shape), 0.0), axis=1, keepdims=True)
    if ny > 1:
        wait_for(slot_by, by_sem)
    total = sums_b[core, x, y]
    for k in range(ny - 1):
        total = total + slot_by[k]
    hidden_b[core, x, y] = gelu(total + bias)

    hb_y_sem, ha_x_sem, pair_ha_sem, pair_hb_sem = (send.receive() for _ in range(4))
    own = hidden_b.at[core, x, y]
    for i in others_y:
        send("hb y", own, own, at_y(i), hb_y_sem)
    if nx > 1:
        wait_for(slot_ax, ax_sem)
    total = sums_a[core, y, x]
    for k in range(nx - 1):
        total = total + slot_ax[k]
    hidden_a[core, y, x] = gelu(total + bias)
    own = hidden_a.at[core, y, x]
    for i in others_x:
        send("ha x", own, own, at_x(i), ha_x_sem)
    if nx > 1:
        wait_for(hidden_a.at[0, 0, pl.ds(0, nx - 1)], ha_x_sem)

    def hidden_view(src, h):
        return hidden_a.at[core, src, pl.ds(h * half_x, half_x)]

    def to_partner(block):
        send("pair ha", block, block, partner, pair_ha_sem)

    if ny == 8:
        ring = gather_two_stages(
            y,
            at_y,
            lambda src: hidden_a.at[core, src],
            lambda src, d: hidden_view(src, int(d < 0)),
            send,
            "ha y",
            to_partner,
        )
    else:
        ring = gather_ring(
            ny, y, at_y, hidden_view, send, "ha y", lambda src, h: to_partner(hidden_view(src, h))
        )
    next(ring, None)
    to_partner(hidden_a.at[core, y])
    if ny > 1:
        wait_for(hidden_b.at[0, 0, pl.ds(0, ny - 1)], hb_y_sem)
    own = hidden_b.at[core, x]
    hb_x = [send("hb x", own, own, at_x(i)) for i in others_x]
    send("pair hb", own, own, partner, pair_hb_sem)
    next(ring, None)
    for k, copy in enumerate(hb_x):
        copy.wait_recv()
        block = hidden_b.at[core, wrap(x - 1 - k, nx)]
        send("pair hb", block, block, partner, pair_hb_sem)
    for _ in ring:
        pass
    wait_for(hidden_b.at[0], pair_hb_sem)
    wait_for(hidden_a.at[0], pair_ha_sem)
    for c in range(CORES):

        def split_hidden(j, _, c=c):
            for i, value in enumerate((hidden_a[c, :, j], hidden_b[c, j])):
                value = value.reshape(core_rows, x_width)
                for k in range(per_x):
                    at = (i * (nz // 2) + j * per_x + k, pl.ds(c * core_rows, core_rows))
                    hidden_h[at], hidden_l[at] = split(value[:, k * LANES : (k + 1) * LANES])
            return 0

        lax.fori_loop(0, nx, split_hidden, 0)

    z_slots = slots_of(nz, PIECES)
    width = 256

    def split_out(i, _):
        for c in range(CORES):
            for j in range(nx):
                row = ((i * nx + j) * CORES + c) * depth
                at = pl.ds(pl.multiple_of(row, depth), depth)
                ch_out_h[at, :], ch_out_l[at, :] = split(ch_out_f[c, j, i])
        return 0

    def split_in(i, _):
        for c in range(CORES):
            for j in range(nx):
                row = ((i * nx + j) * CORES + c) * depth
                at = pl.ds(pl.multiple_of(row, depth), depth)
                ch_in_h[at, :], ch_in_l[at, :] = split(ch_in_f[c, i, j])
        return 0

    def stages(c):
        at = pl.ds(c * chunk_rows, chunk_rows)

        def mixed_ready(dst, dist):
            if c == 0:
                mixed[dst] = dot3(tok_out_h[...], tok_out_l[...], hidden_h[dst], hidden_l[dst], NN)

        def view(ref):
            return lambda i, h: ref.at[i, pl.ds(c * chunk_rows + h * piece_rows, piece_rows)]

        def slot(ref):
            return lambda d, t, h: ref.at[c, z_slots[(d, t, h)]]

        yield from reduce_ring(nz, z, at_z, view(mixed), slot(mixed_slot), send, "mixed", mixed_ready, PIECES)
        kept[z, at, :] = gathered[z, pl.ds(GAINS + c * chunk_rows, chunk_rows), :] + mixed[z, at, :]
        yield from gather_ring(nz, z, at_z, view(kept), send, "kept", pieces=PIECES)
        yield "weights"
        normalize(c, kept, 0, 1)

        def hidden_block(j, _):
            columns = pl.ds(pl.multiple_of(j * width, width), width)
            result = dot3(high[at, :], low[at, :], ch_in_h[:, columns], ch_in_l[:, columns], NN)
            act_h[at, columns], act_l[at, columns] = split(gelu(result + ch_bias_v[:, columns]))
            return 0

        lax.fori_loop(0, hidden_width // width, hidden_block, 0)

        def final_ready(dst, dist):
            wanted_rows = pl.ds(pl.multiple_of(dst * LANES, LANES), LANES)
            final[dst, at, :] = dot3(act_h[at, :], act_l[at, :], ch_out_h[wanted_rows, :], ch_out_l[wanted_rows, :], NT)

        yield from reduce_ring(nz, z, at_z, view(final), slot(final_slot), send, "final", final_ready, PIECES)
        out[at, :] = kept[z, at, :] + final[z, at, :]

    def weights():
        yield next(ring_in_y, None)
        yield next(ring_out_x, None)
        yield next(ring_in_y, None)
        for _ in ring_out_x:
            pass
        yield
        yield next(ring_in_y, None)
        wait_for(ch_out_f.at[0], pair_out_sem)
        lax.fori_loop(0, ny, split_out, 0)
        yield
        for _ in ring_in_y:
            pass
        yield
        wait_for(ch_in_f.at[0], pair_in_sem)
        lax.fori_loop(0, ny, split_in, 0)
        yield

    late = weights()
    chains = [stages(c) for c in range(CHUNKS)]
    step = 0
    while chains:
        for chain in list(chains):
            try:
                if next(chain) == "weights":
                    for _ in late:
                        pass
                    next(chain)
            except StopIteration:
                chains.remove(chain)
        next(late, None)
        step += 1
    send.finish(
        {
            "fields": gathered.at[pl.ds(0, nz - 1)],
            "mixed": mixed.at[pl.ds(0, nz - 1)],
            "kept": kept.at[pl.ds(0, nz - 1)],
            "final": final.at[pl.ds(0, nz - 1)],
            "out y": ch_out_f.at[0, 0, pl.ds(0, ny - 1)],
            "out x": ch_out_f.at[0, pl.ds(0, nx - 1)],
            "in x": ch_in_f.at[0, 0, pl.ds(0, nx - 1)],
            "in y": ch_in_f.at[0, pl.ds(0, ny - 1)],
            "pair in": ch_in_f.at[0],
            "pair out": ch_out_f.at[0],
            "pair a": pair_a,
            "pair b": pair_b,
            "sums y": sums_a.at[0, pl.ds(0, ny - 1)],
            "b x": slot_bx,
            "b y": slot_by,
            "a x": slot_ax,
            "hb y": hidden_b.at[0, 0, pl.ds(0, ny - 1)],
            "hb x": hidden_b.at[0, pl.ds(0, nx - 1)],
            "ha x": hidden_a.at[0, 0, pl.ds(0, nx - 1)],
            "ha y": hidden_a.at[0, pl.ds(0, ny - 1)],
            "pair ha": hidden_a.at[0],
            "pair hb": hidden_b.at[0],
        }
    )


def block(nz, ny, nx, fields, gain_one, tok_in, tok_bias, tok_out, gain_two, ch_in, ch_bias, ch_out):
    rows, hidden_tok = fields.shape[0], tok_in.shape[0]
    depth, hidden_width = ch_in.shape
    channels = nz * LANES
    y_rows = hidden_tok // (CORES * ny)
    x_width = channels // (2 * nx)
    z_slots = max(1, len(slots_of(nz, PIECES)))
    piece_rows = rows // (PIECES * CHUNKS)

    def vmem(*shape, kind=F32):
        return pltpu.VMEM(shape, kind)

    scratch = [
        vmem(nz, rows + GAINS, LANES),
        vmem(nz, rows, LANES),
        vmem(rows, channels, kind=BF16),
        vmem(rows, channels, kind=BF16),
        vmem(hidden_tok, rows),
        vmem(hidden_tok, rows, kind=BF16),
        vmem(hidden_tok, rows, kind=BF16),
        vmem(rows, hidden_tok),
        vmem(rows, hidden_tok, kind=BF16),
        vmem(rows, hidden_tok, kind=BF16),
        vmem(CORES, ny, nx, y_rows, x_width),
        vmem(CORES, nx, ny, y_rows, x_width),
        vmem(ny, nx, y_rows, x_width),
        vmem(nx, ny, y_rows, x_width),
        vmem(max(1, ny - 1), nx, y_rows, x_width),
        vmem(nx - 1, y_rows, x_width),
        vmem(nx - 1, ny, y_rows, x_width),
        vmem(max(1, ny - 1), y_rows, x_width),
        vmem(CORES, ny, nx, y_rows, x_width),
        vmem(CORES, nx, ny, y_rows, x_width),
        vmem(nz, hidden_tok, LANES, kind=BF16),
        vmem(nz, hidden_tok, LANES, kind=BF16),
        vmem(nz, rows, LANES),
        vmem(CHUNKS, z_slots, piece_rows, LANES),
        vmem(CORES, ny, nx, depth, hidden_width),
        vmem(channels, hidden_width, kind=BF16),
        vmem(channels, hidden_width, kind=BF16),
        vmem(CORES, nx, ny, depth, hidden_width),
        vmem(channels, hidden_width, kind=BF16),
        vmem(channels, hidden_width, kind=BF16),
        vmem(rows, hidden_width, kind=BF16),
        vmem(rows, hidden_width, kind=BF16),
        vmem(nz, rows, LANES),
        vmem(CHUNKS, z_slots, piece_rows, LANES),
        vmem(1, hidden_tok),
        vmem(1, hidden_width),
        pltpu.SemaphoreType.DMA((9,)),
        pltpu.SemaphoreType.DMA((SENDS,)),
        pltpu.SemaphoreType.DMA((RECEIVES,)),
    ]
    hbm = pl.BlockSpec(memory_space=pltpu.HBM)
    return pl.pallas_call(
        functools.partial(kernel, nz, ny, nx),
        out_shape=jax.ShapeDtypeStruct((rows, LANES), F32),
        in_specs=[hbm] * 9,
        out_specs=pl.BlockSpec(memory_space=pltpu.VMEM),
        scratch_shapes=scratch,
        compiler_params=pltpu.CompilerParams(
            collective_id=0, has_side_effects=True, vmem_limit_bytes=48 * 1024 * 1024
        ),
    )(
        *(
            pltpu.with_memory_space_constraint(argument, pltpu.HBM)
            for argument in (
                fields,
                gain_one.reshape(1, LANES),
                gain_two.reshape(1, LANES),
                tok_in,
                tok_bias,
                tok_out,
                ch_in,
                ch_bias,
                ch_out.T,
            )
        )
    )


def solution(mesh):
    in_specs = (
        P("tok", "ch"),
        P("ch"),
        P("ch", "tok"),
        P("ch"),
        P("tok", "ch"),
        P("ch"),
        P("tok", "ch"),
        P("ch"),
        P("ch", "tok"),
    )
    body = functools.partial(block, mesh.shape["ch"], NY, NX)
    return jax.shard_map(body, mesh=mesh, in_specs=in_specs, out_specs=P("tok", "ch"), check_vma=False)
```

```python
import functools

import jax
import jax.numpy as jnp
from jax import lax
from jax.experimental import pallas as pl
from jax.experimental.pallas import tpu as pltpu
from jax.sharding import PartitionSpec as P

NY, NX = 8, 4
CORES = 2
CHUNKS = 2
PIECES = 4
MESH = pl.DeviceIdType.MESH
F32, BF16 = jnp.float32, jnp.bfloat16
EPSILON = 1e-05
LANES = 128
GAINS = 8


def split(value):
    high = value.astype(BF16)
    return high, (value - high.astype(F32)).astype(BF16)


def gelu(value):
    return 0.5 * value * (1.0 + lax.erf(value * 0.7071067811865476))


def dot3(a_high, a_low, b_high, b_low, dims):
    def one(a, b):
        return lax.dot_general(a, b, (dims, ((), ())), preferred_element_type=F32)

    return one(a_high, b_high) + (one(a_high, b_low) + one(a_low, b_high))


NN = ((1,), (0,))
NT = ((1,), (1,))
SENDS, RECEIVES = 22, 188


class Sender:
    def __init__(self, send_sem, recv_sem):
        self.send_sem, self.recv_sem = send_sem, recv_sem
        self.groups, self.named, self.receives = {}, {}, 0

    def receive(self):
        self.receives += 1
        return self.recv_sem.at[self.receives - 1]

    def shared(self, name):
        def of(key):
            if (name, key) not in self.named:
                self.named[(name, key)] = self.receive()
            return self.named[(name, key)]

        return of

    def __call__(self, group, src, dst, device, recv=None):
        copy = pltpu.make_async_remote_copy(
            src_ref=src,
            dst_ref=dst,
            send_sem=self.send_sem.at[self.groups.setdefault(group, len(self.groups))],
            recv_sem=self.receive() if recv is None else recv,
            device_id=device,
            device_id_type=MESH,
        )
        copy.start()
        return copy

    def finish(self, sizes):
        for group, k in self.groups.items():
            wait_for(sizes[group], self.send_sem.at[k])


def wait_for(like, sem):
    pltpu.make_async_copy(like, like, sem).wait()


def wrap(value, n):
    return lax.rem(value + 2 * n, n)


def gather_ring(
    n, me, device, view, send, group, arrived=lambda src, h: None, pieces=2, recv=lambda key: None, source=None
):
    half = n // 2
    flight = {}

    def take(d, s, h):
        flight.pop((d, s, h)).wait_recv()
        arrived(wrap(me - d * s, n), h)

    for s in range(1, half + 1):
        for h in range(pieces):
            first = source(h) if s == 1 and source else None
            for d in (1, -1):
                if s == half and (d == 1) != (h < pieces // 2):
                    continue
                if s > 1:
                    take(d, s - 1, h)
                block = view(wrap(me - d * (s - 1), n), h)
                flight[(d, s, h)] = send(
                    group, block if first is None else first, block, device(wrap(me + d, n)), recv((d, s, h))
                )
        yield
    for key in sorted(flight, key=lambda k: (k[1], k[2])):
        take(*key)


def reduce_ring(
    n, me, device, part, slot, send, group, ready=lambda dst, dist: None, pieces=2, recv=lambda key: None
):
    half = n // 2
    flight = {}

    def add(dst, d, t, h):
        flight.pop((d, t, h)).wait_recv()
        part(dst, h)[...] += slot(d, t, h)[...]

    for t in range(1, half + 1):
        dist = half + 1 - t
        ready(wrap(me + dist, n), dist)
        if dist != half:
            ready(wrap(me - dist, n), -dist)
        for h in range(pieces):
            for d in (1, -1):
                first = 1 if (d == 1) == (h < pieces // 2) else 2
                if t < first:
                    continue
                dst = wrap(me + d * dist, n)
                if t > first:
                    add(dst, d, t - 1, h)
                flight[(d, t, h)] = send(
                    group, part(dst, h), slot(d, t, h), device(wrap(me + d, n)), recv((d, t, h))
                )
        yield
    ready(me, 0)
    for key in sorted(flight, key=lambda k: (k[1], k[2])):
        add(me, *key)


def reduce_two_stages(me, device, whole, half, slot, send, group, ready):
    n = 8
    flight = {}
    ready(wrap(me + 4, n), 4)
    for d in (1, -1):
        dst = wrap(me + 4 * d, n)
        flight[(d, 4)] = send(group, half(dst, d), slot(d, 4), device(wrap(me + 2 * d, n)))
    for d in (1, -1):
        dst = wrap(me + 3 * d, n)
        ready(dst, 3 * d)
        flight[(d, 3)] = send(group, whole(dst), slot(d, 3), device(wrap(me + d, n)))
    for d in (1, -1):
        dst = wrap(me + d, n)
        ready(dst, d)
        flight[(d, 1)] = send(group, whole(dst), slot(d, 1), device(dst))
    for d in (1, -1):
        ready(wrap(me + 2 * d, n), 2 * d)
    ready(me, 0)
    yield
    for d in (1, -1):
        dst = wrap(me + 2 * d, n)
        flight[(d, 3)].wait_recv()
        flight[(d, 4)].wait_recv()
        whole(dst)[...] += slot(d, 3)[...]
        half(dst, d)[...] += slot(d, 4)[...]
        flight[(d, 2)] = send(group, whole(dst), slot(d, 2), device(dst))
    yield
    for k in (1, 2):
        for d in (1, -1):
            flight[(d, k)].wait_recv()
            whole(me)[...] += slot(d, k)[...]


def gather_two_stages(me, device, whole, half, send, group, arrived):
    n = 8
    flight = {}
    own = whole(me)
    for k in (2, 1):
        for d in (1, -1):
            flight[(d, k)] = send(group, own, own, device(wrap(me + k * d, n)))
    yield
    for d in (1, -1):
        src = wrap(me - 2 * d, n)
        flight[(d, 2)].wait_recv()
        block = half(src, d)
        flight[(d, 4)] = send(group, block, block, device(wrap(me + 2 * d, n)))
        block = whole(src)
        flight[(d, 3)] = send(group, block, block, device(wrap(me + d, n)))
        arrived(block)
    for d in (1, -1):
        flight[(d, 1)].wait_recv()
        arrived(whole(wrap(me - d, n)))
    yield
    for d in (1, -1):
        flight[(d, 3)].wait_recv()
        arrived(whole(wrap(me - 3 * d, n)))
    for d in (1, -1):
        flight[(d, 4)].wait_recv()
        arrived(half(wrap(me - 4 * d, n), d))


def slots_of(n, pieces=2):
    half = n // 2
    places = {}
    for t in range(1, half + 1):
        for h in range(pieces):
            for d in (1, -1):
                if t >= (1 if (d == 1) == (h < pieces // 2) else 2):
                    places[(d, t, h)] = len(places)
    return places


def kernel(
    nz, ny, nx,
    fields, gain_one, gain_two, tok_in, tok_bias, tok_out, ch_in, ch_bias, ch_out,
    out,
    gathered, kept, high, low, tok_in_f, tok_in_h, tok_in_l, tok_out_f, tok_out_h, tok_out_l,
    sums_a, sums_b, pair_a, pair_b, slot_a, slot_ax, slot_bx, slot_by, hidden_a, hidden_b, hidden_h, hidden_l,
    mixed, mixed_slot, ch_in_f, ch_in_h, ch_in_l, ch_out_f, ch_out_h, ch_out_l, act_h, act_l,
    final, final_slot, tok_bias_v, ch_bias_v, local_sem, send_sem, recv_sem,
):
    tok, z = lax.axis_index("tok"), lax.axis_index("ch")
    core = lax.rem(tok, CORES)
    chip = lax.div(tok, CORES)
    x, y = lax.rem(chip, nx), lax.div(chip, nx)
    other = 1 - core
    rows = fields.shape[0]
    chunk_rows = rows // CHUNKS
    piece_rows = chunk_rows // PIECES
    channels = nz * LANES
    x_width = sums_a.shape[4]
    per_x = x_width // LANES
    y_rows = sums_a.shape[3]
    core_rows = ny * y_rows
    depth, hidden_width = ch_in.shape
    half_x, half_y = nx // 2, ny // 2

    def at_z(i):
        return (tok, i)

    def at_y(i):
        return ((i * nx + x) * CORES + core, z)

    def at_x(i):
        return ((y * nx + i) * CORES + core, z)

    partner = ((y * nx + x) * CORES + other, z)
    others_x = [wrap(x + k, nx) for k in range(1, nx)]
    others_y = [wrap(y + k, ny) for k in range(1, ny)]

    local = [
        pltpu.make_async_copy(source, target, local_sem.at[k])
        for k, (source, target) in enumerate(
            [
                (gain_one, gathered.at[z, pl.ds(chunk_rows, 1)]),
                (gain_two, gathered.at[z, pl.ds(chunk_rows + 1, 1)]),
                (
                    fields.at[pl.ds(chunk_rows - piece_rows, piece_rows)],
                    gathered.at[z, pl.ds(chunk_rows - piece_rows, piece_rows)],
                ),
                (ch_in, ch_in_f.at[core, y, x]),
                (ch_out, ch_out_f.at[core, x, y]),
                (tok_in, tok_in_f),
                (tok_out, tok_out_f),
                (tok_bias, tok_bias_v.at[0]),
                (ch_bias, ch_bias_v.at[0]),
                (
                    fields.at[pl.ds(0, chunk_rows - piece_rows)],
                    gathered.at[z, pl.ds(0, chunk_rows - piece_rows)],
                ),
                (
                    fields.at[pl.ds(chunk_rows, rows - chunk_rows)],
                    gathered.at[z, pl.ds(chunk_rows + GAINS, rows - chunk_rows)],
                ),
            ]
        )
    ]
    for copy in local:
        copy.start()

    peers = [partner] + [at_x(i) for i in others_x]
    if ny > 1:
        peers += [at_y(wrap(y + 1, ny)), at_y(wrap(y - 1, ny))]
    if nz > 1:
        peers += [at_z(wrap(z + 1, nz)), at_z(wrap(z - 1, nz))]
    barrier = pltpu.get_barrier_semaphore()
    for peer in peers:
        pl.semaphore_signal(barrier, inc=1, device_id=peer, device_id_type=MESH)
    pl.semaphore_wait(barrier, len(peers))

    send = Sender(send_sem, recv_sem)

    def field_view(c):
        def view(src, h):
            start = c * (chunk_rows + GAINS) + h * piece_rows
            extra = GAINS if (c, h) == (0, PIECES - 1) else 0
            return gathered.at[src, pl.ds(start, piece_rows + extra)]

        return view

    def field_source(c):
        def source(h):
            if (c, h) == (0, PIECES - 1):
                for copy in local[:3]:
                    copy.wait()
                return field_view(c)(z, h)
            return fields.at[pl.ds(c * chunk_rows + h * piece_rows, piece_rows)]

        return source

    half_depth = depth // 2

    def depth_half(ref):
        return lambda src, h: ref.at[core, src, :, pl.ds(h * half_depth, half_depth)]

    pair_in_sem, pair_out_sem = send.receive(), send.receive()

    def in_to_partner(src, h):
        block = depth_half(ch_in_f)(src, h)
        send("pair in", block, block, partner, pair_in_sem)

    def out_to_partner(src, h):
        block = depth_half(ch_out_f)(src, h)
        send("pair out", block, block, partner, pair_out_sem)

    gather_sems = [send.shared(f"gather {c}") for c in range(CHUNKS)]
    reduce_sems = [send.shared(f"reduce {c}") for c in range(CHUNKS)]
    ring_fields = [
        gather_ring(
            nz, z, at_z, field_view(c), send, "fields", pieces=PIECES, recv=gather_sems[c], source=field_source(c)
        )
        for c in range(CHUNKS)
    ]
    ring_out_y = gather_ring(
        ny, y, at_y, lambda src, h: ch_out_f.at[core, x, src, pl.ds(h * half_depth, half_depth)], send, "out y"
    )
    ring_in_y = gather_ring(ny, y, at_y, depth_half(ch_in_f), send, "in y", in_to_partner)
    ring_out_x = gather_ring(nx, x, at_x, depth_half(ch_out_f), send, "out x", out_to_partner)

    for ring in ring_fields:
        next(ring, None)
    for copy in local[3:5]:
        copy.wait()
    own = ch_in_f.at[core, y, x]
    in_x_sem = send.receive()
    for i in others_x:
        send("in x", own, own, at_x(i), in_x_sem)
    next(ring_out_y, None)
    for copy in local[5:]:
        copy.wait()

    def split_rows(source, high_ref, low_ref, step=32):
        def body(i, _):
            at = pl.ds(pl.multiple_of(i * step, step), step)
            high_ref[at, :], low_ref[at, :] = split(source[at, :])
            return 0

        lax.fori_loop(0, source.shape[0] // step, body, 0)

    split_rows(tok_in_f, tok_in_h, tok_in_l)
    split_rows(tok_out_f, tok_out_h, tok_out_l)

    def normalize(c, source, offset, gain_row):
        at = pl.ds(c * chunk_rows, chunk_rows)

        def block(j):
            return source[j, pl.ds(c * chunk_rows + offset, chunk_rows), :]

        total = block(0)
        for j in range(1, nz):
            total = total + block(j)
        mean = jnp.sum(total, axis=1, keepdims=True) * (1.0 / channels)
        total = jnp.square(block(0) - mean)
        for j in range(1, nz):
            total = total + jnp.square(block(j) - mean)
        spread = jnp.sum(total, axis=1, keepdims=True) * (1.0 / channels)
        scale = lax.rsqrt(spread + EPSILON)
        for j in range(nz):
            gain = gathered[j, pl.ds(gain_row, 1), :]
            columns = pl.ds(j * LANES, LANES)
            high[at, columns], low[at, columns] = split((block(j) - mean) * scale * gain)

    for s in range(2, nz // 2 + 1):
        for ring in ring_fields:
            next(ring)
        next(ring_out_y, None)
    for c, ring in enumerate(ring_fields):
        for _ in ring:
            pass
        if c == CHUNKS - 1:
            for _ in ring_out_y:
                pass
            if nx > 1:
                wait_for(ch_in_f.at[0, 0, pl.ds(0, nx - 1)], in_x_sem)
            for h in (0, 1):
                in_to_partner(y, h)
                out_to_partner(x, h)
            next(ring_in_y, None)
            next(ring_out_x, None)
        normalize(c, gathered, c * GAINS, chunk_rows)

    def hidden_sums(which, i):
        at = pl.ds(pl.multiple_of(which * core_rows, core_rows), core_rows)

        def body(j, _):
            start = i * (channels // 2) + 2 * j * x_width
            columns = pl.ds(pl.multiple_of(start, LANES), 2 * x_width)
            result = dot3(tok_in_h[at, :], tok_in_l[at, :], high[:, columns], low[:, columns], NN)
            for k in range(2):
                for r in range(ny):
                    piece = result[r * y_rows : (r + 1) * y_rows, k * x_width : (k + 1) * x_width]
                    if i == 0:
                        sums_a[which, r, 2 * j + k] = piece
                    else:
                        sums_b[which, 2 * j + k, r] = piece
            return 0

        lax.fori_loop(0, half_x, body, 0)

    offsets = [4, 3, -3, 1, -1, 2, -2, 0] if ny == 8 else [0]
    if ny != 8:
        for dist in range(1, half_y):
            offsets = [dist, -dist] + offsets
        offsets = ([half_y] if half_y else []) + offsets
    far, near = ([4, 3, -3, 2], [-2, 1, -1, 0]) if ny == 8 else (list(range(1, ny)), [0])
    hidden_sums(other, 1)
    pair_b_copies = []
    for i in others_x + [x]:
        pair_b_copies.append(send("pair b", sums_b.at[other, i], pair_b.at[i], partner))
    hidden_sums(other, 0)
    pair_sums = {}
    for k in offsets:
        dst = wrap(y + k, ny)
        pair_sums[k] = send("pair a", sums_a.at[other, dst], pair_a.at[dst], partner)
    hidden_sums(core, 1)
    bx_sems = [send.receive(), send.receive()]
    by_sem, ax_sem = send.receive(), send.receive()
    for k, i in enumerate(others_x):
        pair_b_copies[k].wait_recv()
        sums_b[core, i] += pair_b[i]
    for sem, group in zip(bx_sems, (far, near)):
        for k, i in enumerate(others_x):
            for o in group:
                dst = wrap(y + o, ny)
                send("b x", sums_b.at[core, i, dst], slot_bx.at[k, dst], at_x(i), sem)
    hidden_sums(core, 0)

    def sums_ready(dst, dist):
        pair_sums[dist].wait_recv()
        sums_a[core, dst] += pair_a[dst]

    y_slots = slots_of(ny)

    def sums_half(dst, h):
        return sums_a.at[core, dst, pl.ds(h * half_x, half_x)]

    if ny == 8:
        places = {1: 0, 2: 2, 3: 4}

        def y_slot(d, k):
            if k == 4:
                return slot_a.at[6, pl.ds((d < 0) * half_x, half_x)]
            return slot_a.at[places[k] + (d < 0)]

        ring = reduce_two_stages(
            y,
            at_y,
            lambda dst: sums_a.at[core, dst],
            lambda dst, d: sums_half(dst, int(d < 0)),
            y_slot,
            send,
            "sums y",
            sums_ready,
        )
    else:
        ring = reduce_ring(
            ny,
            y,
            at_y,
            sums_half,
            lambda d, t, h: slot_a.at[y_slots[(d, t, h)] // 2, pl.ds((y_slots[(d, t, h)] % 2) * half_x, half_x)],
            send,
            "sums y",
            sums_ready,
        )
    next(ring, None)
    pair_b_copies[-1].wait_recv()
    sums_b[core, x] += pair_b[x]

    def add_bx(sem, group):
        if nx > 1 and group:
            wait_for(slot_bx.at[:, pl.ds(0, len(group))], sem)
        for o in group:
            dst = wrap(y + o, ny)
            total = sums_b[core, x, dst]
            for k in range(nx - 1):
                total = total + slot_bx[k, dst]
            sums_b[core, x, dst] = total
            if o:
                send("b y", sums_b.at[core, x, dst], slot_by.at[wrap(o, ny) - 1], at_y(dst), by_sem)

    next(ring, None)
    add_bx(bx_sems[0], far)
    add_bx(bx_sems[1], near)
    for _ in ring:
        pass
    for k, i in enumerate(others_x):
        send("a x", sums_a.at[core, y, i], slot_ax.at[k], at_x(i), ax_sem)
    first = core * core_rows + y * y_rows
    shape = (y_rows, tok_bias_v.shape[1])
    wanted = lax.broadcasted_iota(jnp.int32, shape, 1) == lax.broadcasted_iota(jnp.int32, shape, 0) + first
    bias = jnp.sum(jnp.where(wanted, jnp.broadcast_to(tok_bias_v[...], shape), 0.0), axis=1, keepdims=True)
    if ny > 1:
        wait_for(slot_by, by_sem)
    total = sums_b[core, x, y]
    for k in range(ny - 1):
        total = total + slot_by[k]
    hidden_b[core, x, y] = gelu(total + bias)

    ha_x_sem, pair_ha_sem, pair_hb_sem = (send.receive() for _ in range(3))
    hb_y_sem = send.receive()
    hb_x_sems = [send.receive() for _ in others_x]
    own = hidden_b.at[core, x, y]
    for i in others_y:
        send("hb y", own, own, at_y(i), hb_y_sem)
    if nx > 1:
        wait_for(slot_ax, ax_sem)
    total = sums_a[core, y, x]
    for k in range(nx - 1):
        total = total + slot_ax[k]
    hidden_a[core, y, x] = gelu(total + bias)
    own = hidden_a.at[core, y, x]
    for i in others_x:
        send("ha x", own, own, at_x(i), ha_x_sem)
    if nx > 1:
        wait_for(hidden_a.at[0, 0, pl.ds(0, nx - 1)], ha_x_sem)

    def hidden_view(src, h):
        return hidden_a.at[core, src, pl.ds(h * half_x, half_x)]

    def to_partner(block):
        send("pair ha", block, block, partner, pair_ha_sem)

    if ny == 8:
        ring = gather_two_stages(
            y,
            at_y,
            lambda src: hidden_a.at[core, src],
            lambda src, d: hidden_view(src, int(d < 0)),
            send,
            "ha y",
            to_partner,
        )
    else:
        ring = gather_ring(
            ny, y, at_y, hidden_view, send, "ha y", lambda src, h: to_partner(hidden_view(src, h))
        )
    next(ring, None)
    to_partner(hidden_a.at[core, y])
    if ny > 1:
        wait_for(hidden_b.at[0, 0, pl.ds(0, ny - 1)], hb_y_sem)
    own = hidden_b.at[core, x]
    for i, sem in zip(others_x, hb_x_sems):
        send("hb x", own, own, at_x(i), sem)
    send("pair hb", own, own, partner, pair_hb_sem)
    next(ring, None)
    for k, sem in enumerate(hb_x_sems):
        block = hidden_b.at[core, wrap(x - 1 - k, nx)]
        wait_for(block, sem)
        send("pair hb", block, block, partner, pair_hb_sem)
    for _ in ring:
        pass
    wait_for(hidden_b.at[0], pair_hb_sem)
    wait_for(hidden_a.at[0], pair_ha_sem)
    for c in range(CORES):

        def split_hidden(j, _, c=c):
            for i, value in enumerate((hidden_a[c, :, j], hidden_b[c, j])):
                value = value.reshape(core_rows, x_width)
                for k in range(per_x):
                    at = (i * (nz // 2) + j * per_x + k, pl.ds(c * core_rows, core_rows))
                    hidden_h[at], hidden_l[at] = split(value[:, k * LANES : (k + 1) * LANES])
            return 0

        lax.fori_loop(0, nx, split_hidden, 0)

    z_slots = slots_of(nz, PIECES)
    width = 256

    def split_out(i, _):
        for c in range(CORES):
            for j in range(nx):
                row = ((i * nx + j) * CORES + c) * depth
                at = pl.ds(pl.multiple_of(row, depth), depth)
                ch_out_h[at, :], ch_out_l[at, :] = split(ch_out_f[c, j, i])
        return 0

    def split_in(i, _):
        for c in range(CORES):
            for j in range(nx):
                row = ((i * nx + j) * CORES + c) * depth
                at = pl.ds(pl.multiple_of(row, depth), depth)
                ch_in_h[at, :], ch_in_l[at, :] = split(ch_in_f[c, i, j])
        return 0

    def stages(c):
        at = pl.ds(c * chunk_rows, chunk_rows)

        def mixed_ready(dst, dist):
            if c == 0:
                mixed[dst] = dot3(tok_out_h[...], tok_out_l[...], hidden_h[dst], hidden_l[dst], NN)

        def view(ref):
            return lambda i, h: ref.at[i, pl.ds(c * chunk_rows + h * piece_rows, piece_rows)]

        def slot(ref):
            return lambda d, t, h: ref.at[c, z_slots[(d, t, h)]]

        yield from reduce_ring(nz, z, at_z, view(mixed), slot(mixed_slot), send, "mixed", mixed_ready, PIECES, reduce_sems[c])
        kept[z, at, :] = gathered[z, pl.ds(c * (chunk_rows + GAINS), chunk_rows), :] + mixed[z, at, :]
        yield from gather_ring(nz, z, at_z, view(kept), send, "kept", pieces=PIECES, recv=gather_sems[c])
        yield "weights"
        normalize(c, kept, 0, chunk_rows + 1)

        def hidden_block(j, _):
            columns = pl.ds(pl.multiple_of(j * width, width), width)
            result = dot3(high[at, :], low[at, :], ch_in_h[:, columns], ch_in_l[:, columns], NN)
            act_h[at, columns], act_l[at, columns] = split(gelu(result + ch_bias_v[:, columns]))
            return 0

        lax.fori_loop(0, hidden_width // width, hidden_block, 0)

        def final_ready(dst, dist):
            wanted_rows = pl.ds(pl.multiple_of(dst * LANES, LANES), LANES)
            final[dst, at, :] = dot3(act_h[at, :], act_l[at, :], ch_out_h[wanted_rows, :], ch_out_l[wanted_rows, :], NT)

        yield from reduce_ring(nz, z, at_z, view(final), slot(final_slot), send, "final", final_ready, PIECES, reduce_sems[c])
        out[at, :] = kept[z, at, :] + final[z, at, :]

    def weights():
        yield next(ring_in_y, None)
        yield next(ring_out_x, None)
        yield next(ring_in_y, None)
        for _ in ring_out_x:
            pass
        yield
        yield next(ring_in_y, None)
        wait_for(ch_out_f.at[0], pair_out_sem)
        lax.fori_loop(0, ny, split_out, 0)
        yield
        for _ in ring_in_y:
            pass
        yield
        wait_for(ch_in_f.at[0], pair_in_sem)
        lax.fori_loop(0, ny, split_in, 0)
        yield

    late = weights()
    chains = [stages(c) for c in range(CHUNKS)]
    step = 0
    while chains:
        for chain in list(chains):
            try:
                if next(chain) == "weights":
                    for _ in late:
                        pass
                    next(chain)
            except StopIteration:
                chains.remove(chain)
        next(late, None)
        step += 1
    send.finish(
        {
            "fields": gathered.at[pl.ds(0, nz - 1)],
            "mixed": mixed.at[pl.ds(0, nz - 1)],
            "kept": kept.at[pl.ds(0, nz - 1)],
            "final": final.at[pl.ds(0, nz - 1)],
            "out y": ch_out_f.at[0, 0, pl.ds(0, ny - 1)],
            "out x": ch_out_f.at[0, pl.ds(0, nx - 1)],
            "in x": ch_in_f.at[0, 0, pl.ds(0, nx - 1)],
            "in y": ch_in_f.at[0, pl.ds(0, ny - 1)],
            "pair in": ch_in_f.at[0],
            "pair out": ch_out_f.at[0],
            "pair a": pair_a,
            "pair b": pair_b,
            "sums y": sums_a.at[0, pl.ds(0, ny - 1)],
            "b x": slot_bx,
            "b y": slot_by,
            "a x": slot_ax,
            "hb y": hidden_b.at[0, 0, pl.ds(0, ny - 1)],
            "hb x": hidden_b.at[0, pl.ds(0, nx - 1)],
            "ha x": hidden_a.at[0, 0, pl.ds(0, nx - 1)],
            "ha y": hidden_a.at[0, pl.ds(0, ny - 1)],
            "pair ha": hidden_a.at[0],
            "pair hb": hidden_b.at[0],
        }
    )


def block(nz, ny, nx, fields, gain_one, tok_in, tok_bias, tok_out, gain_two, ch_in, ch_bias, ch_out):
    rows, hidden_tok = fields.shape[0], tok_in.shape[0]
    depth, hidden_width = ch_in.shape
    channels = nz * LANES
    y_rows = hidden_tok // (CORES * ny)
    x_width = channels // (2 * nx)
    z_slots = max(1, len(slots_of(nz, PIECES)))
    piece_rows = rows // (PIECES * CHUNKS)

    def vmem(*shape, kind=F32):
        return pltpu.VMEM(shape, kind)

    scratch = [
        vmem(nz, rows + GAINS, LANES),
        vmem(nz, rows, LANES),
        vmem(rows, channels, kind=BF16),
        vmem(rows, channels, kind=BF16),
        vmem(hidden_tok, rows),
        vmem(hidden_tok, rows, kind=BF16),
        vmem(hidden_tok, rows, kind=BF16),
        vmem(rows, hidden_tok),
        vmem(rows, hidden_tok, kind=BF16),
        vmem(rows, hidden_tok, kind=BF16),
        vmem(CORES, ny, nx, y_rows, x_width),
        vmem(CORES, nx, ny, y_rows, x_width),
        vmem(ny, nx, y_rows, x_width),
        vmem(nx, ny, y_rows, x_width),
        vmem(max(1, ny - 1), nx, y_rows, x_width),
        vmem(nx - 1, y_rows, x_width),
        vmem(nx - 1, ny, y_rows, x_width),
        vmem(max(1, ny - 1), y_rows, x_width),
        vmem(CORES, ny, nx, y_rows, x_width),
        vmem(CORES, nx, ny, y_rows, x_width),
        vmem(nz, hidden_tok, LANES, kind=BF16),
        vmem(nz, hidden_tok, LANES, kind=BF16),
        vmem(nz, rows, LANES),
        vmem(CHUNKS, z_slots, piece_rows, LANES),
        vmem(CORES, ny, nx, depth, hidden_width),
        vmem(channels, hidden_width, kind=BF16),
        vmem(channels, hidden_width, kind=BF16),
        vmem(CORES, nx, ny, depth, hidden_width),
        vmem(channels, hidden_width, kind=BF16),
        vmem(channels, hidden_width, kind=BF16),
        vmem(rows, hidden_width, kind=BF16),
        vmem(rows, hidden_width, kind=BF16),
        vmem(nz, rows, LANES),
        vmem(CHUNKS, z_slots, piece_rows, LANES),
        vmem(1, hidden_tok),
        vmem(1, hidden_width),
        pltpu.SemaphoreType.DMA((11,)),
        pltpu.SemaphoreType.DMA((SENDS,)),
        pltpu.SemaphoreType.DMA((RECEIVES,)),
    ]
    hbm = pl.BlockSpec(memory_space=pltpu.HBM)
    return pl.pallas_call(
        functools.partial(kernel, nz, ny, nx),
        out_shape=jax.ShapeDtypeStruct((rows, LANES), F32),
        in_specs=[hbm] * 9,
        out_specs=pl.BlockSpec(memory_space=pltpu.VMEM),
        scratch_shapes=scratch,
        compiler_params=pltpu.CompilerParams(
            collective_id=0, has_side_effects=True, vmem_limit_bytes=48 * 1024 * 1024
        ),
    )(
        *(
            pltpu.with_memory_space_constraint(argument, pltpu.HBM)
            for argument in (
                fields,
                gain_one.reshape(1, LANES),
                gain_two.reshape(1, LANES),
                tok_in,
                tok_bias,
                tok_out,
                ch_in,
                ch_bias,
                ch_out.T,
            )
        )
    )


def solution(mesh):
    in_specs = (
        P("tok", "ch"),
        P("ch"),
        P("ch", "tok"),
        P("ch"),
        P("tok", "ch"),
        P("ch"),
        P("tok", "ch"),
        P("ch"),
        P("ch", "tok"),
    )
    body = functools.partial(block, mesh.shape["ch"], NY, NX)
    return jax.shard_map(body, mesh=mesh, in_specs=in_specs, out_specs=P("tok", "ch"), check_vma=False)
```

```python
import functools

import jax
import jax.numpy as jnp
from jax import lax
from jax.experimental import pallas as pl
from jax.experimental.pallas import tpu as pltpu
from jax.sharding import PartitionSpec as P

NY, NX = 8, 4
CORES = 2
CHUNKS = 2
PIECES = 4
MESH = pl.DeviceIdType.MESH
F32, BF16 = jnp.float32, jnp.bfloat16
EPSILON = 1e-05
LANES = 128
GAINS = 8


def split(value):
    high = value.astype(BF16)
    return high, (value - high.astype(F32)).astype(BF16)


def gelu(value):
    return 0.5 * value * (1.0 + lax.erf(value * 0.7071067811865476))


def dot3(a_high, a_low, b_high, b_low, dims):
    def one(a, b):
        return lax.dot_general(a, b, (dims, ((), ())), preferred_element_type=F32)

    return one(a_high, b_high) + (one(a_high, b_low) + one(a_low, b_high))


NN = ((1,), (0,))
NT = ((1,), (1,))
SENDS, RECEIVES = 22, 188


class Sender:
    def __init__(self, send_sem, recv_sem):
        self.send_sem, self.recv_sem = send_sem, recv_sem
        self.groups, self.named, self.receives = {}, {}, 0

    def receive(self):
        self.receives += 1
        return self.recv_sem.at[self.receives - 1]

    def shared(self, name):
        def of(key):
            if (name, key) not in self.named:
                self.named[(name, key)] = self.receive()
            return self.named[(name, key)]

        return of

    def __call__(self, group, src, dst, device, recv=None):
        copy = pltpu.make_async_remote_copy(
            src_ref=src,
            dst_ref=dst,
            send_sem=self.send_sem.at[self.groups.setdefault(group, len(self.groups))],
            recv_sem=self.receive() if recv is None else recv,
            device_id=device,
            device_id_type=MESH,
        )
        copy.start()
        return copy

    def finish(self, sizes):
        for group, k in self.groups.items():
            wait_for(sizes[group], self.send_sem.at[k])


def wait_for(like, sem):
    pltpu.make_async_copy(like, like, sem).wait()


def wrap(value, n):
    return lax.rem(value + 2 * n, n)


def gather_ring(
    n, me, device, view, send, group, arrived=lambda src, h: None, pieces=2, recv=lambda key: None, source=None
):
    half = n // 2
    flight = {}

    def take(d, s, h):
        flight.pop((d, s, h)).wait_recv()
        arrived(wrap(me - d * s, n), h)

    for s in range(1, half + 1):
        for h in range(pieces):
            first = source(h) if s == 1 and source else None
            for d in (1, -1):
                if s == half and (d == 1) != (h < pieces // 2):
                    continue
                if s > 1:
                    take(d, s - 1, h)
                block = view(wrap(me - d * (s - 1), n), h)
                flight[(d, s, h)] = send(
                    group, block if first is None else first, block, device(wrap(me + d, n)), recv((d, s, h))
                )
        yield
    for key in sorted(flight, key=lambda k: (k[1], k[2])):
        take(*key)


def reduce_ring(
    n, me, device, part, slot, send, group, ready=lambda blocks: None, pieces=2, recv=lambda key: None
):
    half = n // 2
    flight = {}

    def add(dst, d, t, h):
        flight.pop((d, t, h)).wait_recv()
        part(dst, h)[...] += slot(d, t, h)[...]

    for t in range(1, half + 1):
        dist = half + 1 - t
        ready([wrap(me + k, n) for k in ((dist,) if dist == half else (dist, -dist))])
        for h in range(pieces):
            for d in (1, -1):
                first = 1 if (d == 1) == (h < pieces // 2) else 2
                if t < first:
                    continue
                dst = wrap(me + d * dist, n)
                if t > first:
                    add(dst, d, t - 1, h)
                flight[(d, t, h)] = send(
                    group, part(dst, h), slot(d, t, h), device(wrap(me + d, n)), recv((d, t, h))
                )
        yield
    ready([me])
    for key in sorted(flight, key=lambda k: (k[1], k[2])):
        add(me, *key)


def reduce_two_stages(me, device, whole, half, slot, send, group, ready):
    n = 8
    flight = {}
    ready(wrap(me + 4, n), 4)
    for d in (1, -1):
        dst = wrap(me + 4 * d, n)
        flight[(d, 4)] = send(group, half(dst, d), slot(d, 4), device(wrap(me + 2 * d, n)))
    for d in (1, -1):
        dst = wrap(me + 3 * d, n)
        ready(dst, 3 * d)
        flight[(d, 3)] = send(group, whole(dst), slot(d, 3), device(wrap(me + d, n)))
    for d in (1, -1):
        dst = wrap(me + d, n)
        ready(dst, d)
        flight[(d, 1)] = send(group, whole(dst), slot(d, 1), device(dst))
    for d in (1, -1):
        ready(wrap(me + 2 * d, n), 2 * d)
    ready(me, 0)
    yield
    for d in (1, -1):
        dst = wrap(me + 2 * d, n)
        flight[(d, 3)].wait_recv()
        flight[(d, 4)].wait_recv()
        whole(dst)[...] += slot(d, 3)[...]
        half(dst, d)[...] += slot(d, 4)[...]
        flight[(d, 2)] = send(group, whole(dst), slot(d, 2), device(dst))
    yield
    for k in (1, 2):
        for d in (1, -1):
            flight[(d, k)].wait_recv()
            whole(me)[...] += slot(d, k)[...]


def gather_two_stages(me, device, whole, half, send, group, arrived):
    n = 8
    flight = {}
    own = whole(me)
    for k in (2, 1):
        for d in (1, -1):
            flight[(d, k)] = send(group, own, own, device(wrap(me + k * d, n)))
    yield
    for d in (1, -1):
        src = wrap(me - 2 * d, n)
        flight[(d, 2)].wait_recv()
        block = half(src, d)
        flight[(d, 4)] = send(group, block, block, device(wrap(me + 2 * d, n)))
        block = whole(src)
        flight[(d, 3)] = send(group, block, block, device(wrap(me + d, n)))
        arrived(block)
    for d in (1, -1):
        flight[(d, 1)].wait_recv()
        arrived(whole(wrap(me - d, n)))
    yield
    for d in (1, -1):
        flight[(d, 3)].wait_recv()
        arrived(whole(wrap(me - 3 * d, n)))
    for d in (1, -1):
        flight[(d, 4)].wait_recv()
        arrived(half(wrap(me - 4 * d, n), d))


def slots_of(n, pieces=2):
    half = n // 2
    places = {}
    for t in range(1, half + 1):
        for h in range(pieces):
            for d in (1, -1):
                if t >= (1 if (d == 1) == (h < pieces // 2) else 2):
                    places[(d, t, h)] = len(places)
    return places


def kernel(
    nz, ny, nx,
    fields, gain_one, gain_two, tok_in, tok_bias, tok_out, ch_in, ch_bias, ch_out,
    out,
    gathered, kept, high, low, tok_in_f, tok_in_h, tok_in_l, tok_out_f, tok_out_h, tok_out_l,
    sums_a, sums_b, pair_a, pair_b, slot_a, slot_ax, slot_bx, slot_by, hidden_a, hidden_b, hidden_h, hidden_l,
    mixed, mixed_slot, ch_in_f, ch_in_h, ch_in_l, ch_out_f, ch_out_h, ch_out_l, act_h, act_l,
    final, final_slot, tok_bias_v, ch_bias_v, local_sem, send_sem, recv_sem,
):
    tok, z = lax.axis_index("tok"), lax.axis_index("ch")
    core = lax.rem(tok, CORES)
    chip = lax.div(tok, CORES)
    x, y = lax.rem(chip, nx), lax.div(chip, nx)
    other = 1 - core
    rows = fields.shape[0]
    chunk_rows = rows // CHUNKS
    piece_rows = chunk_rows // PIECES
    channels = nz * LANES
    x_width = sums_a.shape[4]
    per_x = x_width // LANES
    y_rows = sums_a.shape[3]
    core_rows = ny * y_rows
    depth, hidden_width = ch_in.shape
    half_x, half_y = nx // 2, ny // 2

    def at_z(i):
        return (tok, i)

    def at_y(i):
        return ((i * nx + x) * CORES + core, z)

    def at_x(i):
        return ((y * nx + i) * CORES + core, z)

    partner = ((y * nx + x) * CORES + other, z)
    others_x = [wrap(x + k, nx) for k in range(1, nx)]
    others_y = [wrap(y + k, ny) for k in range(1, ny)]

    local = [
        pltpu.make_async_copy(source, target, local_sem.at[k])
        for k, (source, target) in enumerate(
            [
                (gain_one, gathered.at[z, pl.ds(chunk_rows, 1)]),
                (gain_two, gathered.at[z, pl.ds(chunk_rows + 1, 1)]),
                (
                    fields.at[pl.ds(chunk_rows - piece_rows, piece_rows)],
                    gathered.at[z, pl.ds(chunk_rows - piece_rows, piece_rows)],
                ),
                (ch_in, ch_in_f.at[core, y, x]),
                (ch_out, ch_out_f.at[core, x, y]),
                (tok_in, tok_in_f),
                (tok_out, tok_out_f),
                (tok_bias, tok_bias_v.at[0]),
                (ch_bias, ch_bias_v.at[0]),
                (
                    fields.at[pl.ds(0, chunk_rows - piece_rows)],
                    gathered.at[z, pl.ds(0, chunk_rows - piece_rows)],
                ),
                (
                    fields.at[pl.ds(chunk_rows, rows - chunk_rows)],
                    gathered.at[z, pl.ds(chunk_rows + GAINS, rows - chunk_rows)],
                ),
            ]
        )
    ]
    for copy in local:
        copy.start()

    peers = [partner] + [at_x(i) for i in others_x]
    if ny > 1:
        peers += [at_y(wrap(y + 1, ny)), at_y(wrap(y - 1, ny))]
    if nz > 1:
        peers += [at_z(wrap(z + 1, nz)), at_z(wrap(z - 1, nz))]
    barrier = pltpu.get_barrier_semaphore()
    for peer in peers:
        pl.semaphore_signal(barrier, inc=1, device_id=peer, device_id_type=MESH)
    pl.semaphore_wait(barrier, len(peers))

    send = Sender(send_sem, recv_sem)

    def field_view(c):
        def view(src, h):
            start = c * (chunk_rows + GAINS) + h * piece_rows
            extra = GAINS if (c, h) == (0, PIECES - 1) else 0
            return gathered.at[src, pl.ds(start, piece_rows + extra)]

        return view

    def field_source(c):
        def source(h):
            if (c, h) == (0, PIECES - 1):
                for copy in local[:3]:
                    copy.wait()
                return field_view(c)(z, h)
            return fields.at[pl.ds(c * chunk_rows + h * piece_rows, piece_rows)]

        return source

    half_depth = depth // 2

    def depth_half(ref):
        return lambda src, h: ref.at[core, src, :, pl.ds(h * half_depth, half_depth)]

    pair_in_sem, pair_out_sem = send.receive(), send.receive()

    def in_to_partner(src, h):
        block = depth_half(ch_in_f)(src, h)
        send("pair in", block, block, partner, pair_in_sem)

    def out_to_partner(src, h):
        block = depth_half(ch_out_f)(src, h)
        send("pair out", block, block, partner, pair_out_sem)

    gather_sems = [send.shared(f"gather {c}") for c in range(CHUNKS)]
    reduce_sems = [send.shared(f"reduce {c}") for c in range(CHUNKS)]
    ring_fields = [
        gather_ring(
            nz, z, at_z, field_view(c), send, "fields", pieces=PIECES, recv=gather_sems[c], source=field_source(c)
        )
        for c in range(CHUNKS)
    ]
    ring_out_y = gather_ring(
        ny, y, at_y, lambda src, h: ch_out_f.at[core, x, src, pl.ds(h * half_depth, half_depth)], send, "out y"
    )
    ring_in_y = gather_ring(ny, y, at_y, depth_half(ch_in_f), send, "in y", in_to_partner)
    ring_out_x = gather_ring(nx, x, at_x, depth_half(ch_out_f), send, "out x", out_to_partner)

    for ring in ring_fields:
        next(ring, None)
    for copy in local[3:5]:
        copy.wait()
    own = ch_in_f.at[core, y, x]
    in_x_sem = send.receive()
    for i in others_x:
        send("in x", own, own, at_x(i), in_x_sem)
    next(ring_out_y, None)
    for copy in local[5:]:
        copy.wait()

    def split_rows(source, high_ref, low_ref, step=32):
        def body(i, _):
            at = pl.ds(pl.multiple_of(i * step, step), step)
            high_ref[at, :], low_ref[at, :] = split(source[at, :])
            return 0

        lax.fori_loop(0, source.shape[0] // step, body, 0)

    split_rows(tok_in_f, tok_in_h, tok_in_l)
    split_rows(tok_out_f, tok_out_h, tok_out_l)

    def normalize(c, source, offset, gain_row):
        at = pl.ds(c * chunk_rows, chunk_rows)

        def block(j):
            return source[j, pl.ds(c * chunk_rows + offset, chunk_rows), :]

        total = block(0)
        for j in range(1, nz):
            total = total + block(j)
        mean = jnp.sum(total, axis=1, keepdims=True) * (1.0 / channels)
        total = jnp.square(block(0) - mean)
        for j in range(1, nz):
            total = total + jnp.square(block(j) - mean)
        spread = jnp.sum(total, axis=1, keepdims=True) * (1.0 / channels)
        scale = lax.rsqrt(spread + EPSILON)
        for j in range(nz):
            gain = gathered[j, pl.ds(gain_row, 1), :]
            columns = pl.ds(j * LANES, LANES)
            high[at, columns], low[at, columns] = split((block(j) - mean) * scale * gain)

    for s in range(2, nz // 2 + 1):
        for ring in ring_fields:
            next(ring)
        next(ring_out_y, None)
        if s == min(3, nz // 2):
            if nx > 1:
                wait_for(ch_in_f.at[0, 0, pl.ds(0, nx - 1)], in_x_sem)
            for h in (0, 1):
                in_to_partner(y, h)
            next(ring_in_y, None)
    for c, ring in enumerate(ring_fields):
        for _ in ring:
            pass
        if c == CHUNKS - 1:
            for _ in ring_out_y:
                pass
            for h in (0, 1):
                out_to_partner(x, h)
        normalize(c, gathered, c * GAINS, chunk_rows)

    def hidden_sums(which, i):
        at = pl.ds(pl.multiple_of(which * core_rows, core_rows), core_rows)

        def body(j, _):
            start = i * (channels // 2) + 2 * j * x_width
            columns = pl.ds(pl.multiple_of(start, LANES), 2 * x_width)
            result = dot3(tok_in_h[at, :], tok_in_l[at, :], high[:, columns], low[:, columns], NN)
            for k in range(2):
                for r in range(ny):
                    piece = result[r * y_rows : (r + 1) * y_rows, k * x_width : (k + 1) * x_width]
                    if i == 0:
                        sums_a[which, r, 2 * j + k] = piece
                    else:
                        sums_b[which, 2 * j + k, r] = piece
            return 0

        lax.fori_loop(0, half_x, body, 0)

    offsets = [4, 3, -3, 1, -1, 2, -2, 0] if ny == 8 else [0]
    if ny != 8:
        for dist in range(1, half_y):
            offsets = [dist, -dist] + offsets
        offsets = ([half_y] if half_y else []) + offsets
    far, near = ([4, 3, -3, 2], [-2, 1, -1, 0]) if ny == 8 else (list(range(1, ny)), [0])
    hidden_sums(other, 0)
    pair_sums = {}
    for k in offsets:
        dst = wrap(y + k, ny)
        pair_sums[k] = send("pair a", sums_a.at[other, dst], pair_a.at[dst], partner)
    hidden_sums(other, 1)
    pair_b_copies = []
    for i in others_x + [x]:
        pair_b_copies.append(send("pair b", sums_b.at[other, i], pair_b.at[i], partner))
    hidden_sums(core, 0)

    def sums_ready(dst, dist):
        pair_sums[dist].wait_recv()
        sums_a[core, dst] += pair_a[dst]

    y_slots = slots_of(ny)

    def sums_half(dst, h):
        return sums_a.at[core, dst, pl.ds(h * half_x, half_x)]

    if ny == 8:
        places = {1: 0, 2: 2, 3: 4}

        def y_slot(d, k):
            if k == 4:
                return slot_a.at[6, pl.ds((d < 0) * half_x, half_x)]
            return slot_a.at[places[k] + (d < 0)]

        ring = reduce_two_stages(
            y,
            at_y,
            lambda dst: sums_a.at[core, dst],
            lambda dst, d: sums_half(dst, int(d < 0)),
            y_slot,
            send,
            "sums y",
            sums_ready,
        )
    else:
        ring = reduce_ring(
            ny,
            y,
            at_y,
            sums_half,
            lambda d, t, h: slot_a.at[y_slots[(d, t, h)] // 2, pl.ds((y_slots[(d, t, h)] % 2) * half_x, half_x)],
            send,
            "sums y",
        )
    if ny != 8:
        for k in offsets:
            sums_ready(wrap(y + k, ny), k)
    next(ring, None)
    hidden_sums(core, 1)
    bx_sems = [send.receive(), send.receive()]
    by_sem, ax_sem = send.receive(), send.receive()
    for k, i in enumerate(others_x):
        pair_b_copies[k].wait_recv()
        sums_b[core, i] += pair_b[i]
    for sem, group in zip(bx_sems, (far, near)):
        for k, i in enumerate(others_x):
            for o in group:
                dst = wrap(y + o, ny)
                send("b x", sums_b.at[core, i, dst], slot_bx.at[k, dst], at_x(i), sem)
    pair_b_copies[-1].wait_recv()
    sums_b[core, x] += pair_b[x]

    def add_bx(sem, group):
        if nx > 1 and group:
            wait_for(slot_bx.at[:, pl.ds(0, len(group))], sem)
        for o in group:
            dst = wrap(y + o, ny)
            total = sums_b[core, x, dst]
            for k in range(nx - 1):
                total = total + slot_bx[k, dst]
            sums_b[core, x, dst] = total
            if o:
                send("b y", sums_b.at[core, x, dst], slot_by.at[wrap(o, ny) - 1], at_y(dst), by_sem)

    next(ring, None)
    add_bx(bx_sems[0], far)
    add_bx(bx_sems[1], near)
    for _ in ring:
        pass
    for k, i in enumerate(others_x):
        send("a x", sums_a.at[core, y, i], slot_ax.at[k], at_x(i), ax_sem)
    first = core * core_rows + y * y_rows
    shape = (y_rows, tok_bias_v.shape[1])
    wanted = lax.broadcasted_iota(jnp.int32, shape, 1) == lax.broadcasted_iota(jnp.int32, shape, 0) + first
    bias = jnp.sum(jnp.where(wanted, jnp.broadcast_to(tok_bias_v[...], shape), 0.0), axis=1, keepdims=True)
    if ny > 1:
        wait_for(slot_by, by_sem)
    total = sums_b[core, x, y]
    for k in range(ny - 1):
        total = total + slot_by[k]
    hidden_b[core, x, y] = gelu(total + bias)

    ha_x_sem, pair_ha_sem, pair_hb_sem = (send.receive() for _ in range(3))
    hb_y_sem = send.receive()
    hb_x_sems = [send.receive() for _ in others_x]
    own = hidden_b.at[core, x, y]
    for i in others_y:
        send("hb y", own, own, at_y(i), hb_y_sem)
    if nx > 1:
        wait_for(slot_ax, ax_sem)
    total = sums_a[core, y, x]
    for k in range(nx - 1):
        total = total + slot_ax[k]
    hidden_a[core, y, x] = gelu(total + bias)
    own = hidden_a.at[core, y, x]
    for i in others_x:
        send("ha x", own, own, at_x(i), ha_x_sem)
    if nx > 1:
        wait_for(hidden_a.at[0, 0, pl.ds(0, nx - 1)], ha_x_sem)

    def hidden_view(src, h):
        return hidden_a.at[core, src, pl.ds(h * half_x, half_x)]

    def to_partner(block):
        send("pair ha", block, block, partner, pair_ha_sem)

    if ny == 8:
        ring = gather_two_stages(
            y,
            at_y,
            lambda src: hidden_a.at[core, src],
            lambda src, d: hidden_view(src, int(d < 0)),
            send,
            "ha y",
            to_partner,
        )
    else:
        ring = gather_ring(
            ny, y, at_y, hidden_view, send, "ha y", lambda src, h: to_partner(hidden_view(src, h))
        )
    next(ring, None)
    to_partner(hidden_a.at[core, y])
    if ny > 1:
        wait_for(hidden_b.at[0, 0, pl.ds(0, ny - 1)], hb_y_sem)
    own = hidden_b.at[core, x]
    for i, sem in zip(others_x, hb_x_sems):
        send("hb x", own, own, at_x(i), sem)
    send("pair hb", own, own, partner, pair_hb_sem)
    next(ring, None)
    for k, sem in enumerate(hb_x_sems):
        block = hidden_b.at[core, wrap(x - 1 - k, nx)]
        wait_for(block, sem)
        send("pair hb", block, block, partner, pair_hb_sem)
    for _ in ring:
        pass
    wait_for(hidden_b.at[0], pair_hb_sem)
    wait_for(hidden_a.at[0], pair_ha_sem)
    for c in range(CORES):

        def split_hidden(j, _, c=c):
            for i, value in enumerate((hidden_a[c, :, j], hidden_b[c, j])):
                value = value.reshape(core_rows, x_width)
                for k in range(per_x):
                    at = (i * (nz // 2) + j * per_x + k, pl.ds(c * core_rows, core_rows))
                    hidden_h[at], hidden_l[at] = split(value[:, k * LANES : (k + 1) * LANES])
            return 0

        lax.fori_loop(0, nx, split_hidden, 0)

    z_slots = slots_of(nz, PIECES)
    width = 256

    def split_out(i, _):
        for c in range(CORES):
            for j in range(nx):
                row = ((i * nx + j) * CORES + c) * depth
                at = pl.ds(pl.multiple_of(row, depth), depth)
                ch_out_h[at, :], ch_out_l[at, :] = split(ch_out_f[c, j, i])
        return 0

    def split_in(i, _):
        for c in range(CORES):
            for j in range(nx):
                row = ((i * nx + j) * CORES + c) * depth
                at = pl.ds(pl.multiple_of(row, depth), depth)
                ch_in_h[at, :], ch_in_l[at, :] = split(ch_in_f[c, i, j])
        return 0

    def stages(c):
        at = pl.ds(c * chunk_rows, chunk_rows)

        def mixed_ready(blocks):
            if c == 0:
                right = [jnp.concatenate([ref[dst] for dst in blocks], axis=1) for ref in (hidden_h, hidden_l)]
                result = dot3(tok_out_h[...], tok_out_l[...], *right, NN)
                for k, dst in enumerate(blocks):
                    mixed[dst] = result[:, k * LANES : (k + 1) * LANES]

        def view(ref):
            return lambda i, h: ref.at[i, pl.ds(c * chunk_rows + h * piece_rows, piece_rows)]

        def slot(ref):
            return lambda d, t, h: ref.at[c, z_slots[(d, t, h)]]

        yield from reduce_ring(nz, z, at_z, view(mixed), slot(mixed_slot), send, "mixed", mixed_ready, PIECES, reduce_sems[c])
        kept[z, at, :] = gathered[z, pl.ds(c * (chunk_rows + GAINS), chunk_rows), :] + mixed[z, at, :]
        yield from gather_ring(nz, z, at_z, view(kept), send, "kept", pieces=PIECES, recv=gather_sems[c])
        yield "weights"
        normalize(c, kept, 0, chunk_rows + 1)

        def hidden_block(j, _):
            columns = pl.ds(pl.multiple_of(j * width, width), width)
            result = dot3(high[at, :], low[at, :], ch_in_h[:, columns], ch_in_l[:, columns], NN)
            act_h[at, columns], act_l[at, columns] = split(gelu(result + ch_bias_v[:, columns]))
            return 0

        lax.fori_loop(0, hidden_width // width, hidden_block, 0)

        def final_ready(blocks):
            wanted = [pl.ds(pl.multiple_of(dst * LANES, LANES), LANES) for dst in blocks]
            right = [jnp.concatenate([ref[rows, :] for rows in wanted], axis=0) for ref in (ch_out_h, ch_out_l)]
            result = dot3(act_h[at, :], act_l[at, :], *right, NT)
            for k, dst in enumerate(blocks):
                final[dst, at, :] = result[:, k * LANES : (k + 1) * LANES]

        yield from reduce_ring(nz, z, at_z, view(final), slot(final_slot), send, "final", final_ready, PIECES, reduce_sems[c])
        out[at, :] = kept[z, at, :] + final[z, at, :]

    def weights():
        next(ring_out_x, None)
        yield next(ring_in_y, None)
        yield
        yield next(ring_in_y, None)
        yield next(ring_out_x, None)
        yield next(ring_in_y, None)
        for _ in ring_out_x:
            pass
        yield
        for _ in ring_in_y:
            pass
        wait_for(ch_out_f.at[0], pair_out_sem)
        lax.fori_loop(0, ny, split_out, 0)
        yield
        wait_for(ch_in_f.at[0], pair_in_sem)
        lax.fori_loop(0, ny, split_in, 0)
        yield

    late = weights()
    chains = [stages(c) for c in range(CHUNKS)]
    step = 0
    while chains:
        for chain in list(chains):
            try:
                if next(chain) == "weights":
                    for _ in late:
                        pass
                    next(chain)
            except StopIteration:
                chains.remove(chain)
        next(late, None)
        step += 1
    send.finish(
        {
            "fields": gathered.at[pl.ds(0, nz - 1)],
            "mixed": mixed.at[pl.ds(0, nz - 1)],
            "kept": kept.at[pl.ds(0, nz - 1)],
            "final": final.at[pl.ds(0, nz - 1)],
            "out y": ch_out_f.at[0, 0, pl.ds(0, ny - 1)],
            "out x": ch_out_f.at[0, pl.ds(0, nx - 1)],
            "in x": ch_in_f.at[0, 0, pl.ds(0, nx - 1)],
            "in y": ch_in_f.at[0, pl.ds(0, ny - 1)],
            "pair in": ch_in_f.at[0],
            "pair out": ch_out_f.at[0],
            "pair a": pair_a,
            "pair b": pair_b,
            "sums y": sums_a.at[0, pl.ds(0, ny - 1)],
            "b x": slot_bx,
            "b y": slot_by,
            "a x": slot_ax,
            "hb y": hidden_b.at[0, 0, pl.ds(0, ny - 1)],
            "hb x": hidden_b.at[0, pl.ds(0, nx - 1)],
            "ha x": hidden_a.at[0, 0, pl.ds(0, nx - 1)],
            "ha y": hidden_a.at[0, pl.ds(0, ny - 1)],
            "pair ha": hidden_a.at[0],
            "pair hb": hidden_b.at[0],
        }
    )


def block(nz, ny, nx, fields, gain_one, tok_in, tok_bias, tok_out, gain_two, ch_in, ch_bias, ch_out):
    rows, hidden_tok = fields.shape[0], tok_in.shape[0]
    depth, hidden_width = ch_in.shape
    channels = nz * LANES
    y_rows = hidden_tok // (CORES * ny)
    x_width = channels // (2 * nx)
    z_slots = max(1, len(slots_of(nz, PIECES)))
    piece_rows = rows // (PIECES * CHUNKS)

    def vmem(*shape, kind=F32):
        return pltpu.VMEM(shape, kind)

    scratch = [
        vmem(nz, rows + GAINS, LANES),
        vmem(nz, rows, LANES),
        vmem(rows, channels, kind=BF16),
        vmem(rows, channels, kind=BF16),
        vmem(hidden_tok, rows),
        vmem(hidden_tok, rows, kind=BF16),
        vmem(hidden_tok, rows, kind=BF16),
        vmem(rows, hidden_tok),
        vmem(rows, hidden_tok, kind=BF16),
        vmem(rows, hidden_tok, kind=BF16),
        vmem(CORES, ny, nx, y_rows, x_width),
        vmem(CORES, nx, ny, y_rows, x_width),
        vmem(ny, nx, y_rows, x_width),
        vmem(nx, ny, y_rows, x_width),
        vmem(max(1, ny - 1), nx, y_rows, x_width),
        vmem(nx - 1, y_rows, x_width),
        vmem(nx - 1, ny, y_rows, x_width),
        vmem(max(1, ny - 1), y_rows, x_width),
        vmem(CORES, ny, nx, y_rows, x_width),
        vmem(CORES, nx, ny, y_rows, x_width),
        vmem(nz, hidden_tok, LANES, kind=BF16),
        vmem(nz, hidden_tok, LANES, kind=BF16),
        vmem(nz, rows, LANES),
        vmem(CHUNKS, z_slots, piece_rows, LANES),
        vmem(CORES, ny, nx, depth, hidden_width),
        vmem(channels, hidden_width, kind=BF16),
        vmem(channels, hidden_width, kind=BF16),
        vmem(CORES, nx, ny, depth, hidden_width),
        vmem(channels, hidden_width, kind=BF16),
        vmem(channels, hidden_width, kind=BF16),
        vmem(rows, hidden_width, kind=BF16),
        vmem(rows, hidden_width, kind=BF16),
        vmem(nz, rows, LANES),
        vmem(CHUNKS, z_slots, piece_rows, LANES),
        vmem(1, hidden_tok),
        vmem(1, hidden_width),
        pltpu.SemaphoreType.DMA((11,)),
        pltpu.SemaphoreType.DMA((SENDS,)),
        pltpu.SemaphoreType.DMA((RECEIVES,)),
    ]
    hbm = pl.BlockSpec(memory_space=pltpu.HBM)
    return pl.pallas_call(
        functools.partial(kernel, nz, ny, nx),
        out_shape=jax.ShapeDtypeStruct((rows, LANES), F32),
        in_specs=[hbm] * 9,
        out_specs=pl.BlockSpec(memory_space=pltpu.VMEM),
        scratch_shapes=scratch,
        compiler_params=pltpu.CompilerParams(
            collective_id=0, has_side_effects=True, vmem_limit_bytes=48 * 1024 * 1024
        ),
    )(
        *(
            pltpu.with_memory_space_constraint(argument, pltpu.HBM)
            for argument in (
                fields,
                gain_one.reshape(1, LANES),
                gain_two.reshape(1, LANES),
                tok_in,
                tok_bias,
                tok_out,
                ch_in,
                ch_bias,
                ch_out.T,
            )
        )
    )


def solution(mesh):
    in_specs = (
        P("tok", "ch"),
        P("ch"),
        P("ch", "tok"),
        P("ch"),
        P("tok", "ch"),
        P("ch"),
        P("tok", "ch"),
        P("ch"),
        P("ch", "tok"),
    )
    body = functools.partial(block, mesh.shape["ch"], NY, NX)
    return jax.shard_map(body, mesh=mesh, in_specs=in_specs, out_specs=P("tok", "ch"), check_vma=False)
```

```python
import functools

import jax
import jax.numpy as jnp
from jax import lax
from jax.experimental import pallas as pl
from jax.experimental.pallas import tpu as pltpu
from jax.sharding import PartitionSpec as P

NY, NX = 8, 4
CORES = 2
CHUNKS = 2
PIECES = 4
SUM_PIECES = 2
MESH = pl.DeviceIdType.MESH
F32, BF16 = jnp.float32, jnp.bfloat16
EPSILON = 1e-05
LANES = 128
GAINS = 8


def split(value):
    high = value.astype(BF16)
    return high, (value - high.astype(F32)).astype(BF16)


def gelu(value):
    return 0.5 * value * (1.0 + lax.erf(value * 0.7071067811865476))


def dot3(a_high, a_low, b_high, b_low, dims):
    def one(a, b):
        return lax.dot_general(a, b, (dims, ((), ())), preferred_element_type=F32)

    return one(a_high, b_high) + (one(a_high, b_low) + one(a_low, b_high))


NN = ((1,), (0,))
NT = ((1,), (1,))
SENDS, RECEIVES = 22, 160


class Sender:
    def __init__(self, send_sem, recv_sem):
        self.send_sem, self.recv_sem = send_sem, recv_sem
        self.groups, self.named, self.receives = {}, {}, 0

    def receive(self):
        self.receives += 1
        return self.recv_sem.at[self.receives - 1]

    def shared(self, name):
        def of(key):
            if (name, key) not in self.named:
                self.named[(name, key)] = self.receive()
            return self.named[(name, key)]

        return of

    def __call__(self, group, src, dst, device, recv=None):
        copy = pltpu.make_async_remote_copy(
            src_ref=src,
            dst_ref=dst,
            send_sem=self.send_sem.at[self.groups.setdefault(group, len(self.groups))],
            recv_sem=self.receive() if recv is None else recv,
            device_id=device,
            device_id_type=MESH,
        )
        copy.start()
        return copy

    def finish(self, sizes):
        for group, k in self.groups.items():
            wait_for(sizes[group], self.send_sem.at[k])


def wait_for(like, sem):
    pltpu.make_async_copy(like, like, sem).wait()


def wrap(value, n):
    return lax.rem(value + 2 * n, n)


def gather_ring(
    n, me, device, view, send, group, arrived=lambda src, h: None, pieces=2, recv=lambda key: None, source=None
):
    half = n // 2
    flight = {}

    def take(d, s, h):
        flight.pop((d, s, h)).wait_recv()
        arrived(wrap(me - d * s, n), h)

    for s in range(1, half + 1):
        for h in range(pieces):
            first = source(h) if s == 1 and source else None
            for d in (1, -1):
                if s == half and (d == 1) != (h < pieces // 2):
                    continue
                if s > 1:
                    take(d, s - 1, h)
                block = view(wrap(me - d * (s - 1), n), h)
                flight[(d, s, h)] = send(
                    group, block if first is None else first, block, device(wrap(me + d, n)), recv((d, s, h))
                )
        yield
    for key in sorted(flight, key=lambda k: (k[1], k[2])):
        take(*key)


def reduce_ring(
    n, me, device, part, slot, send, group, ready=lambda blocks: None, pieces=2, recv=lambda key: None
):
    half = n // 2
    flight = {}

    def add(dst, d, t, h):
        flight.pop((d, t, h)).wait_recv()
        part(dst, h)[...] += slot(d, t, h)[...]

    for t in range(1, half + 1):
        dist = half + 1 - t
        ready([wrap(me + k, n) for k in ((dist,) if dist == half else (dist, -dist))])
        for h in range(pieces):
            for d in (1, -1):
                first = 1 if (d == 1) == (h < pieces // 2) else 2
                if t < first:
                    continue
                dst = wrap(me + d * dist, n)
                if t > first:
                    add(dst, d, t - 1, h)
                flight[(d, t, h)] = send(
                    group, part(dst, h), slot(d, t, h), device(wrap(me + d, n)), recv((d, t, h))
                )
        yield
    ready([me])
    for key in sorted(flight, key=lambda k: (k[1], k[2])):
        add(me, *key)


def reduce_two_stages(me, device, whole, half, slot, send, group, ready):
    n = 8
    flight = {}
    ready(wrap(me + 4, n), 4)
    for d in (1, -1):
        dst = wrap(me + 4 * d, n)
        flight[(d, 4)] = send(group, half(dst, d), slot(d, 4), device(wrap(me + 2 * d, n)))
    for d in (1, -1):
        dst = wrap(me + 3 * d, n)
        ready(dst, 3 * d)
        flight[(d, 3)] = send(group, whole(dst), slot(d, 3), device(wrap(me + d, n)))
    for d in (1, -1):
        dst = wrap(me + d, n)
        ready(dst, d)
        flight[(d, 1)] = send(group, whole(dst), slot(d, 1), device(dst))
    for d in (1, -1):
        ready(wrap(me + 2 * d, n), 2 * d)
    ready(me, 0)
    yield
    for d in (1, -1):
        dst = wrap(me + 2 * d, n)
        flight[(d, 3)].wait_recv()
        flight[(d, 4)].wait_recv()
        whole(dst)[...] += slot(d, 3)[...]
        half(dst, d)[...] += slot(d, 4)[...]
        flight[(d, 2)] = send(group, whole(dst), slot(d, 2), device(dst))
    yield
    for k in (1, 2):
        for d in (1, -1):
            flight[(d, k)].wait_recv()
            whole(me)[...] += slot(d, k)[...]


def gather_two_stages(me, device, whole, half, send, group, arrived):
    n = 8
    flight = {}
    own = whole(me)
    for k in (2, 1):
        for d in (1, -1):
            flight[(d, k)] = send(group, own, own, device(wrap(me + k * d, n)))
    yield
    for d in (1, -1):
        src = wrap(me - 2 * d, n)
        flight[(d, 2)].wait_recv()
        block = half(src, d)
        flight[(d, 4)] = send(group, block, block, device(wrap(me + 2 * d, n)))
        block = whole(src)
        flight[(d, 3)] = send(group, block, block, device(wrap(me + d, n)))
        arrived(block)
    for d in (1, -1):
        flight[(d, 1)].wait_recv()
        arrived(whole(wrap(me - d, n)))
    yield
    for d in (1, -1):
        flight[(d, 3)].wait_recv()
        arrived(whole(wrap(me - 3 * d, n)))
    for d in (1, -1):
        flight[(d, 4)].wait_recv()
        arrived(half(wrap(me - 4 * d, n), d))


def slots_of(n, pieces=2):
    half = n // 2
    places = {}
    for t in range(1, half + 1):
        for h in range(pieces):
            for d in (1, -1):
                if t >= (1 if (d == 1) == (h < pieces // 2) else 2):
                    places[(d, t, h)] = len(places)
    return places


def kernel(
    nz, ny, nx,
    fields, gain_one, gain_two, tok_in, tok_bias, tok_out, ch_in, ch_bias, ch_out,
    out,
    gathered, kept, high, low, tok_in_f, tok_in_h, tok_in_l, tok_out_f, tok_out_h, tok_out_l,
    sums_a, sums_b, pair_a, pair_b, slot_a, slot_ax, slot_bx, slot_by, hidden_a, hidden_b, hidden_h, hidden_l,
    mixed, mixed_slot, ch_in_f, ch_in_h, ch_in_l, ch_out_f, ch_out_h, ch_out_l, act_h, act_l,
    final, final_slot, tok_bias_v, ch_bias_v, local_sem, send_sem, recv_sem,
):
    tok, z = lax.axis_index("tok"), lax.axis_index("ch")
    core = lax.rem(tok, CORES)
    chip = lax.div(tok, CORES)
    x, y = lax.rem(chip, nx), lax.div(chip, nx)
    other = 1 - core
    rows = fields.shape[0]
    chunk_rows = rows // CHUNKS
    piece_rows = chunk_rows // PIECES
    channels = nz * LANES
    x_width = sums_a.shape[4]
    per_x = x_width // LANES
    y_rows = sums_a.shape[3]
    core_rows = ny * y_rows
    depth, hidden_width = ch_in.shape
    half_x, half_y = nx // 2, ny // 2

    def at_z(i):
        return (tok, i)

    def at_y(i):
        return ((i * nx + x) * CORES + core, z)

    def at_x(i):
        return ((y * nx + i) * CORES + core, z)

    partner = ((y * nx + x) * CORES + other, z)
    others_x = [wrap(x + k, nx) for k in range(1, nx)]
    others_y = [wrap(y + k, ny) for k in range(1, ny)]

    local = [
        pltpu.make_async_copy(source, target, local_sem.at[k])
        for k, (source, target) in enumerate(
            [
                (gain_one, gathered.at[z, pl.ds(chunk_rows, 1)]),
                (gain_two, gathered.at[z, pl.ds(chunk_rows + 1, 1)]),
                (
                    fields.at[pl.ds(chunk_rows - piece_rows, piece_rows)],
                    gathered.at[z, pl.ds(chunk_rows - piece_rows, piece_rows)],
                ),
                (ch_in, ch_in_f.at[core, y, x]),
                (ch_out, ch_out_f.at[core, x, y]),
                (tok_in, tok_in_f),
                (tok_out, tok_out_f),
                (tok_bias, tok_bias_v.at[0]),
                (ch_bias, ch_bias_v.at[0]),
                (
                    fields.at[pl.ds(0, chunk_rows - piece_rows)],
                    gathered.at[z, pl.ds(0, chunk_rows - piece_rows)],
                ),
                (
                    fields.at[pl.ds(chunk_rows, rows - chunk_rows)],
                    gathered.at[z, pl.ds(chunk_rows + GAINS, rows - chunk_rows)],
                ),
            ]
        )
    ]
    for copy in local:
        copy.start()

    peers = [partner] + [at_x(i) for i in others_x]
    if ny > 1:
        peers += [at_y(wrap(y + 1, ny)), at_y(wrap(y - 1, ny))]
    if nz > 1:
        peers += [at_z(wrap(z + 1, nz)), at_z(wrap(z - 1, nz))]
    barrier = pltpu.get_barrier_semaphore()
    for peer in peers:
        pl.semaphore_signal(barrier, inc=1, device_id=peer, device_id_type=MESH)
    pl.semaphore_wait(barrier, len(peers))

    send = Sender(send_sem, recv_sem)

    def field_view(c):
        def view(src, h):
            start = c * (chunk_rows + GAINS) + h * piece_rows
            extra = GAINS if (c, h) == (0, PIECES - 1) else 0
            return gathered.at[src, pl.ds(start, piece_rows + extra)]

        return view

    def field_source(c):
        def source(h):
            if (c, h) == (0, PIECES - 1):
                for copy in local[:3]:
                    copy.wait()
                return field_view(c)(z, h)
            return fields.at[pl.ds(c * chunk_rows + h * piece_rows, piece_rows)]

        return source

    half_depth = depth // 2

    def depth_half(ref):
        return lambda src, h: ref.at[core, src, :, pl.ds(h * half_depth, half_depth)]

    pair_in_sem, pair_out_sem = send.receive(), send.receive()

    def in_to_partner(src, h):
        block = depth_half(ch_in_f)(src, h)
        send("pair in", block, block, partner, pair_in_sem)

    def out_to_partner(src, h):
        block = depth_half(ch_out_f)(src, h)
        send("pair out", block, block, partner, pair_out_sem)

    gather_sems = [send.shared(f"gather {c}") for c in range(CHUNKS)]
    reduce_sems = [send.shared(f"reduce {c}") for c in range(CHUNKS)]
    ring_fields = [
        gather_ring(
            nz, z, at_z, field_view(c), send, "fields", pieces=PIECES, recv=gather_sems[c], source=field_source(c)
        )
        for c in range(CHUNKS)
    ]
    ring_out_y = gather_ring(
        ny, y, at_y, lambda src, h: ch_out_f.at[core, x, src, pl.ds(h * half_depth, half_depth)], send, "out y"
    )
    ring_in_y = gather_ring(ny, y, at_y, depth_half(ch_in_f), send, "in y", in_to_partner)
    ring_out_x = gather_ring(nx, x, at_x, depth_half(ch_out_f), send, "out x", out_to_partner)

    for ring in ring_fields:
        next(ring, None)
    for copy in local[3:5]:
        copy.wait()
    own = ch_in_f.at[core, y, x]
    in_x_sem = send.receive()
    for i in others_x:
        send("in x", own, own, at_x(i), in_x_sem)
    next(ring_out_y, None)
    for copy in local[5:]:
        copy.wait()

    def split_rows(source, high_ref, low_ref, step=32):
        def body(i, _):
            at = pl.ds(pl.multiple_of(i * step, step), step)
            high_ref[at, :], low_ref[at, :] = split(source[at, :])
            return 0

        lax.fori_loop(0, source.shape[0] // step, body, 0)

    split_rows(tok_in_f, tok_in_h, tok_in_l)
    split_rows(tok_out_f, tok_out_h, tok_out_l)

    def normalize(c, source, offset, gain_row):
        at = pl.ds(c * chunk_rows, chunk_rows)

        def block(j):
            return source[j, pl.ds(c * chunk_rows + offset, chunk_rows), :]

        total = block(0)
        for j in range(1, nz):
            total = total + block(j)
        mean = jnp.sum(total, axis=1, keepdims=True) * (1.0 / channels)
        total = jnp.square(block(0) - mean)
        for j in range(1, nz):
            total = total + jnp.square(block(j) - mean)
        spread = jnp.sum(total, axis=1, keepdims=True) * (1.0 / channels)
        scale = lax.rsqrt(spread + EPSILON)
        for j in range(nz):
            gain = gathered[j, pl.ds(gain_row, 1), :]
            columns = pl.ds(j * LANES, LANES)
            high[at, columns], low[at, columns] = split((block(j) - mean) * scale * gain)

    for s in range(2, nz // 2 + 1):
        for ring in ring_fields:
            next(ring)
        next(ring_out_y, None)
        if s == min(3, nz // 2):
            if nx > 1:
                wait_for(ch_in_f.at[0, 0, pl.ds(0, nx - 1)], in_x_sem)
            for h in (0, 1):
                in_to_partner(y, h)
            next(ring_in_y, None)
    for c, ring in enumerate(ring_fields):
        for _ in ring:
            pass
        normalize(c, gathered, c * GAINS, chunk_rows)

    def hidden_sums(which, i):
        at = pl.ds(pl.multiple_of(which * core_rows, core_rows), core_rows)

        def body(j, _):
            start = i * (channels // 2) + 2 * j * x_width
            columns = pl.ds(pl.multiple_of(start, LANES), 2 * x_width)
            result = dot3(tok_in_h[at, :], tok_in_l[at, :], high[:, columns], low[:, columns], NN)
            for k in range(2):
                for r in range(ny):
                    piece = result[r * y_rows : (r + 1) * y_rows, k * x_width : (k + 1) * x_width]
                    if i == 0:
                        sums_a[which, r, 2 * j + k] = piece
                    else:
                        sums_b[which, 2 * j + k, r] = piece
            return 0

        lax.fori_loop(0, half_x, body, 0)

    offsets = [4, 3, -3, 1, -1, 2, -2, 0] if ny == 8 else [0]
    if ny != 8:
        for dist in range(1, half_y):
            offsets = [dist, -dist] + offsets
        offsets = ([half_y] if half_y else []) + offsets
    far, near = ([4, 3, -3, 2], [-2, 1, -1, 0]) if ny == 8 else (list(range(1, ny)), [0])
    hidden_sums(other, 0)
    pair_sums = {}
    for k in offsets:
        dst = wrap(y + k, ny)
        pair_sums[k] = send("pair a", sums_a.at[other, dst], pair_a.at[dst], partner)
    hidden_sums(other, 1)
    pair_b_copies = []
    for i in others_x + [x]:
        pair_b_copies.append(send("pair b", sums_b.at[other, i], pair_b.at[i], partner))
    hidden_sums(core, 0)

    def sums_ready(dst, dist):
        pair_sums[dist].wait_recv()
        sums_a[core, dst] += pair_a[dst]

    y_slots = slots_of(ny)

    def sums_half(dst, h):
        return sums_a.at[core, dst, pl.ds(h * half_x, half_x)]

    if ny == 8:
        places = {1: 0, 2: 2, 3: 4}

        def y_slot(d, k):
            if k == 4:
                return slot_a.at[6, pl.ds((d < 0) * half_x, half_x)]
            return slot_a.at[places[k] + (d < 0)]

        ring = reduce_two_stages(
            y,
            at_y,
            lambda dst: sums_a.at[core, dst],
            lambda dst, d: sums_half(dst, int(d < 0)),
            y_slot,
            send,
            "sums y",
            sums_ready,
        )
    else:
        ring = reduce_ring(
            ny,
            y,
            at_y,
            sums_half,
            lambda d, t, h: slot_a.at[y_slots[(d, t, h)] // 2, pl.ds((y_slots[(d, t, h)] % 2) * half_x, half_x)],
            send,
            "sums y",
        )
    if ny != 8:
        for k in offsets:
            sums_ready(wrap(y + k, ny), k)
    next(ring, None)
    hidden_sums(core, 1)
    bx_sems = [send.receive(), send.receive()]
    by_sem, ax_sem = send.receive(), send.receive()
    for k, i in enumerate(others_x):
        pair_b_copies[k].wait_recv()
        sums_b[core, i] += pair_b[i]
    for sem, group in zip(bx_sems, (far, near)):
        for k, i in enumerate(others_x):
            for o in group:
                dst = wrap(y + o, ny)
                send("b x", sums_b.at[core, i, dst], slot_bx.at[k, dst], at_x(i), sem)
    pair_b_copies[-1].wait_recv()
    sums_b[core, x] += pair_b[x]

    def add_bx(sem, group):
        if nx > 1 and group:
            wait_for(slot_bx.at[:, pl.ds(0, len(group))], sem)
        for o in group:
            dst = wrap(y + o, ny)
            total = sums_b[core, x, dst]
            for k in range(nx - 1):
                total = total + slot_bx[k, dst]
            sums_b[core, x, dst] = total
            if o:
                send("b y", sums_b.at[core, x, dst], slot_by.at[wrap(o, ny) - 1], at_y(dst), by_sem)

    for _ in ring_out_y:
        pass
    for h in (0, 1):
        out_to_partner(x, h)
    next(ring, None)
    add_bx(bx_sems[0], far)
    add_bx(bx_sems[1], near)
    for _ in ring:
        pass
    for k, i in enumerate(others_x):
        send("a x", sums_a.at[core, y, i], slot_ax.at[k], at_x(i), ax_sem)
    first = core * core_rows + y * y_rows
    shape = (y_rows, tok_bias_v.shape[1])
    wanted = lax.broadcasted_iota(jnp.int32, shape, 1) == lax.broadcasted_iota(jnp.int32, shape, 0) + first
    bias = jnp.sum(jnp.where(wanted, jnp.broadcast_to(tok_bias_v[...], shape), 0.0), axis=1, keepdims=True)
    if ny > 1:
        wait_for(slot_by, by_sem)
    total = sums_b[core, x, y]
    for k in range(ny - 1):
        total = total + slot_by[k]
    hidden_b[core, x, y] = gelu(total + bias)

    ha_x_sem, pair_ha_sem, pair_hb_sem = (send.receive() for _ in range(3))
    hb_y_sem = send.receive()
    hb_x_sems = [send.receive() for _ in others_x]
    own = hidden_b.at[core, x, y]
    for i in others_y:
        send("hb y", own, own, at_y(i), hb_y_sem)
    if nx > 1:
        wait_for(slot_ax, ax_sem)
    total = sums_a[core, y, x]
    for k in range(nx - 1):
        total = total + slot_ax[k]
    hidden_a[core, y, x] = gelu(total + bias)
    own = hidden_a.at[core, y, x]
    for i in others_x:
        send("ha x", own, own, at_x(i), ha_x_sem)
    if nx > 1:
        wait_for(hidden_a.at[0, 0, pl.ds(0, nx - 1)], ha_x_sem)

    def hidden_view(src, h):
        return hidden_a.at[core, src, pl.ds(h * half_x, half_x)]

    def to_partner(block):
        send("pair ha", block, block, partner, pair_ha_sem)

    if ny == 8:
        ring = gather_two_stages(
            y,
            at_y,
            lambda src: hidden_a.at[core, src],
            lambda src, d: hidden_view(src, int(d < 0)),
            send,
            "ha y",
            to_partner,
        )
    else:
        ring = gather_ring(
            ny, y, at_y, hidden_view, send, "ha y", lambda src, h: to_partner(hidden_view(src, h))
        )
    next(ring, None)
    to_partner(hidden_a.at[core, y])
    if ny > 1:
        wait_for(hidden_b.at[0, 0, pl.ds(0, ny - 1)], hb_y_sem)
    own = hidden_b.at[core, x]
    for i, sem in zip(others_x, hb_x_sems):
        send("hb x", own, own, at_x(i), sem)
    send("pair hb", own, own, partner, pair_hb_sem)
    next(ring, None)
    for k, sem in enumerate(hb_x_sems):
        block = hidden_b.at[core, wrap(x - 1 - k, nx)]
        wait_for(block, sem)
        send("pair hb", block, block, partner, pair_hb_sem)
    for _ in ring:
        pass
    wait_for(hidden_b.at[0], pair_hb_sem)
    wait_for(hidden_a.at[0], pair_ha_sem)
    for c in range(CORES):

        def split_hidden(j, _, c=c):
            for i, value in enumerate((hidden_a[c, :, j], hidden_b[c, j])):
                value = value.reshape(core_rows, x_width)
                for k in range(per_x):
                    at = (i * (nz // 2) + j * per_x + k, pl.ds(c * core_rows, core_rows))
                    hidden_h[at], hidden_l[at] = split(value[:, k * LANES : (k + 1) * LANES])
            return 0

        lax.fori_loop(0, nx, split_hidden, 0)

    z_slots = slots_of(nz, SUM_PIECES)
    width = 256

    def split_out(i, _):
        for c in range(CORES):
            for j in range(nx):
                row = ((i * nx + j) * CORES + c) * depth
                at = pl.ds(pl.multiple_of(row, depth), depth)
                ch_out_h[at, :], ch_out_l[at, :] = split(ch_out_f[c, j, i])
        return 0

    def split_in(i, _):
        for c in range(CORES):
            for j in range(nx):
                row = ((i * nx + j) * CORES + c) * depth
                at = pl.ds(pl.multiple_of(row, depth), depth)
                ch_in_h[at, :], ch_in_l[at, :] = split(ch_in_f[c, i, j])
        return 0

    def stages(c):
        at = pl.ds(c * chunk_rows, chunk_rows)

        def mixed_ready(blocks):
            if c == 0:
                right = [jnp.concatenate([ref[dst] for dst in blocks], axis=1) for ref in (hidden_h, hidden_l)]
                result = dot3(tok_out_h[...], tok_out_l[...], *right, NN)
                for k, dst in enumerate(blocks):
                    mixed[dst] = result[:, k * LANES : (k + 1) * LANES]

        def view(ref, pieces):
            size = chunk_rows // pieces
            return lambda i, h: ref.at[i, pl.ds(c * chunk_rows + h * size, size)]

        def slot(ref):
            return lambda d, t, h: ref.at[c, z_slots[(d, t, h)]]

        yield from reduce_ring(nz, z, at_z, view(mixed, SUM_PIECES), slot(mixed_slot), send, "mixed", mixed_ready, SUM_PIECES, reduce_sems[c])
        kept[z, at, :] = gathered[z, pl.ds(c * (chunk_rows + GAINS), chunk_rows), :] + mixed[z, at, :]
        yield from gather_ring(nz, z, at_z, view(kept, PIECES), send, "kept", pieces=PIECES, recv=gather_sems[c])
        yield "weights"
        normalize(c, kept, 0, chunk_rows + 1)

        def hidden_block(j, _):
            columns = pl.ds(pl.multiple_of(j * width, width), width)
            result = dot3(high[at, :], low[at, :], ch_in_h[:, columns], ch_in_l[:, columns], NN)
            act_h[at, columns], act_l[at, columns] = split(gelu(result + ch_bias_v[:, columns]))
            return 0

        lax.fori_loop(0, hidden_width // width, hidden_block, 0)

        def final_ready(blocks):
            wanted = [pl.ds(pl.multiple_of(dst * LANES, LANES), LANES) for dst in blocks]
            right = [jnp.concatenate([ref[rows, :] for rows in wanted], axis=0) for ref in (ch_out_h, ch_out_l)]
            result = dot3(act_h[at, :], act_l[at, :], *right, NT)
            for k, dst in enumerate(blocks):
                final[dst, at, :] = result[:, k * LANES : (k + 1) * LANES]

        yield from reduce_ring(nz, z, at_z, view(final, SUM_PIECES), slot(final_slot), send, "final", final_ready, SUM_PIECES, reduce_sems[c])
        out[at, :] = kept[z, at, :] + final[z, at, :]

    def weights():
        next(ring_out_x, None)
        yield next(ring_in_y, None)
        yield
        yield next(ring_in_y, None)
        yield next(ring_out_x, None)
        yield next(ring_in_y, None)
        for _ in ring_out_x:
            pass
        yield
        for _ in ring_in_y:
            pass
        wait_for(ch_out_f.at[0], pair_out_sem)
        lax.fori_loop(0, ny, split_out, 0)
        yield
        wait_for(ch_in_f.at[0], pair_in_sem)
        lax.fori_loop(0, ny, split_in, 0)
        yield

    late = weights()
    chains = [stages(c) for c in range(CHUNKS)]
    step = 0
    while chains:
        for chain in list(chains):
            try:
                if next(chain) == "weights":
                    for _ in late:
                        pass
                    next(chain)
            except StopIteration:
                chains.remove(chain)
        next(late, None)
        step += 1
    send.finish(
        {
            "fields": gathered.at[pl.ds(0, nz - 1)],
            "mixed": mixed.at[pl.ds(0, nz - 1)],
            "kept": kept.at[pl.ds(0, nz - 1)],
            "final": final.at[pl.ds(0, nz - 1)],
            "out y": ch_out_f.at[0, 0, pl.ds(0, ny - 1)],
            "out x": ch_out_f.at[0, pl.ds(0, nx - 1)],
            "in x": ch_in_f.at[0, 0, pl.ds(0, nx - 1)],
            "in y": ch_in_f.at[0, pl.ds(0, ny - 1)],
            "pair in": ch_in_f.at[0],
            "pair out": ch_out_f.at[0],
            "pair a": pair_a,
            "pair b": pair_b,
            "sums y": sums_a.at[0, pl.ds(0, ny - 1)],
            "b x": slot_bx,
            "b y": slot_by,
            "a x": slot_ax,
            "hb y": hidden_b.at[0, 0, pl.ds(0, ny - 1)],
            "hb x": hidden_b.at[0, pl.ds(0, nx - 1)],
            "ha x": hidden_a.at[0, 0, pl.ds(0, nx - 1)],
            "ha y": hidden_a.at[0, pl.ds(0, ny - 1)],
            "pair ha": hidden_a.at[0],
            "pair hb": hidden_b.at[0],
        }
    )


def block(nz, ny, nx, fields, gain_one, tok_in, tok_bias, tok_out, gain_two, ch_in, ch_bias, ch_out):
    rows, hidden_tok = fields.shape[0], tok_in.shape[0]
    depth, hidden_width = ch_in.shape
    channels = nz * LANES
    y_rows = hidden_tok // (CORES * ny)
    x_width = channels // (2 * nx)
    z_slots = max(1, len(slots_of(nz, SUM_PIECES)))
    piece_rows = rows // (SUM_PIECES * CHUNKS)

    def vmem(*shape, kind=F32):
        return pltpu.VMEM(shape, kind)

    scratch = [
        vmem(nz, rows + GAINS, LANES),
        vmem(nz, rows, LANES),
        vmem(rows, channels, kind=BF16),
        vmem(rows, channels, kind=BF16),
        vmem(hidden_tok, rows),
        vmem(hidden_tok, rows, kind=BF16),
        vmem(hidden_tok, rows, kind=BF16),
        vmem(rows, hidden_tok),
        vmem(rows, hidden_tok, kind=BF16),
        vmem(rows, hidden_tok, kind=BF16),
        vmem(CORES, ny, nx, y_rows, x_width),
        vmem(CORES, nx, ny, y_rows, x_width),
        vmem(ny, nx, y_rows, x_width),
        vmem(nx, ny, y_rows, x_width),
        vmem(max(1, ny - 1), nx, y_rows, x_width),
        vmem(nx - 1, y_rows, x_width),
        vmem(nx - 1, ny, y_rows, x_width),
        vmem(max(1, ny - 1), y_rows, x_width),
        vmem(CORES, ny, nx, y_rows, x_width),
        vmem(CORES, nx, ny, y_rows, x_width),
        vmem(nz, hidden_tok, LANES, kind=BF16),
        vmem(nz, hidden_tok, LANES, kind=BF16),
        vmem(nz, rows, LANES),
        vmem(CHUNKS, z_slots, piece_rows, LANES),
        vmem(CORES, ny, nx, depth, hidden_width),
        vmem(channels, hidden_width, kind=BF16),
        vmem(channels, hidden_width, kind=BF16),
        vmem(CORES, nx, ny, depth, hidden_width),
        vmem(channels, hidden_width, kind=BF16),
        vmem(channels, hidden_width, kind=BF16),
        vmem(rows, hidden_width, kind=BF16),
        vmem(rows, hidden_width, kind=BF16),
        vmem(nz, rows, LANES),
        vmem(CHUNKS, z_slots, piece_rows, LANES),
        vmem(1, hidden_tok),
        vmem(1, hidden_width),
        pltpu.SemaphoreType.DMA((11,)),
        pltpu.SemaphoreType.DMA((SENDS,)),
        pltpu.SemaphoreType.DMA((RECEIVES,)),
    ]
    hbm = pl.BlockSpec(memory_space=pltpu.HBM)
    return pl.pallas_call(
        functools.partial(kernel, nz, ny, nx),
        out_shape=jax.ShapeDtypeStruct((rows, LANES), F32),
        in_specs=[hbm] * 9,
        out_specs=pl.BlockSpec(memory_space=pltpu.VMEM),
        scratch_shapes=scratch,
        compiler_params=pltpu.CompilerParams(
            collective_id=0, has_side_effects=True, vmem_limit_bytes=48 * 1024 * 1024
        ),
    )(
        *(
            pltpu.with_memory_space_constraint(argument, pltpu.HBM)
            for argument in (
                fields,
                gain_one.reshape(1, LANES),
                gain_two.reshape(1, LANES),
                tok_in,
                tok_bias,
                tok_out,
                ch_in,
                ch_bias,
                ch_out.T,
            )
        )
    )


def solution(mesh):
    in_specs = (
        P("tok", "ch"),
        P("ch"),
        P("ch", "tok"),
        P("ch"),
        P("tok", "ch"),
        P("ch"),
        P("tok", "ch"),
        P("ch"),
        P("ch", "tok"),
    )
    body = functools.partial(block, mesh.shape["ch"], NY, NX)
    return jax.shard_map(body, mesh=mesh, in_specs=in_specs, out_specs=P("tok", "ch"), check_vma=False)
```
